128 devices in a mesh: col: 8 (over y, core), row: 16 (over z, x).
Axes of the slice: x: 4, y: 4, z: 4, core: 2. Of those that a mesh axis runs over, the one named last changes fastest.
Arguments:
- tokens: bfloat16 [4096, 2880], P('row'), may hold values from -6 to 6
- moe_gain: bfloat16 [2880], replicated, may hold values from 0.5 to 1.5
- route_ids: int32 [4096, 4], P('row'), may hold values from 0 to 63, all different within a row; in each aligned block of 256 rows (0 to 255, 256 to 511, ...) at most 24 rows name the same one
- route_weight: float32 [4096, 4], P('row'), may hold values from 0.1 to 1
- w_gate: bfloat16 [64, 2880, 2880], P('row', None, 'col'), may hold values from -0.109375 to 0.109375
- w_up: bfloat16 [64, 2880, 2880], P('row', None, 'col'), may hold values from -0.109375 to 0.109375
- w_down: bfloat16 [64, 2880, 2880], P('row', 'col'), may hold values from -0.109375 to 0.109375
- next_gain: bfloat16 [2880], replicated, may hold values from 0.5 to 1.5
- next_gate: bfloat16 [2880, 128], P(None, 'col'), may hold values from -2 to 2
- next_ids: int32 [4096, 4], P('row'), may hold values from 0 to 127, all different within a row
Outputs:
- mixed: bfloat16 [4096, 2880], P('row', 'col')
- next_logprob: float32 [4096, 4], P('row')
The draws below stay inside these ranges and needn't reach their ends.
Inputs may be any that keep to these rules, and one draw needn't show every extreme that they name: `route_ids`: among the 256 tokens of one index of row, no expert is picked more than 24 times, a bound that some block reaches; a token's picks differ. `next_ids`: A token's picks differ.
All inputs are finite; a program needn't handle non-finite values.
Results may differ from the reference program's by a relative error of at most 0.0095.
Values may be sent and summed in bfloat16 or wider, within the bound.
No kernel may reach another device: no remote copies, remote signals or barrier semaphores. Data moves between devices by JAX's collectives and lax.ppermute only.
A program may use at most 128 MiB of HBM per device.

```python
import math
import jax
import jax.numpy as jnp
import numpy as np
from jax import lax

D = 2880
FF = 2880
EXPERTS = 64
NEXT_EXPERTS = 128
TOP = 4
TOK_ROW = 256
CAP = 24
TOKENS = 4096
N_COL = 8
N_ROW = 16


def joint_draw(key):
    keys = jax.random.split(jax.random.fold_in(key, 7), 3)
    tokens = jax.random.truncated_normal(keys[0], -6.0, 6.0, (TOKENS, D), jnp.float32)
    column_scale = jnp.exp(jax.random.uniform(keys[1], (NEXT_EXPERTS,), jnp.float32, 0.0, math.log(10.0)))
    router = jax.random.truncated_normal(keys[2], -4.0, 4.0, (D, NEXT_EXPERTS), jnp.float32)
    router = router * column_scale[None, :] / math.sqrt(D)
    return (tokens, router)


def draw_tokens(key, part):
    return joint_draw(key)[0].astype(jnp.bfloat16)


def draw_next_gate(key, part):
    return jnp.clip(joint_draw(key)[1], -2.0, 2.0).astype(jnp.bfloat16)


def shard_levels(own_key, dims, cuts, smallest, high):
    gain, own = 1.0, jax.random.fold_in(own_key, 6)
    for position, blocks in cuts:
        heights = jnp.exp(jax.random.uniform(jax.random.fold_in(own, position), (blocks,), jnp.float32, smallest / len(cuts), high / len(cuts)))
        gain = gain * jnp.repeat(heights, dims[position] // blocks).reshape([-1 if axis == position else 1 for axis in range(len(dims))])
    return gain


def different_ones(rng, rows, count, top, lift):
    ranking = jax.random.permutation(jax.random.fold_in(rng, 1), count)
    boost = ranking
    for power in range(3):
        boost = boost * boost // count
    boost = boost * lift // count
    lots = jax.random.randint(jax.random.fold_in(rng, 2), (rows, count), 0, 4096) + boost
    sure = jax.random.permutation(jax.random.fold_in(rng, 3), rows)[jnp.arange(count) % rows]
    lots = jnp.where(jnp.arange(rows)[:, None] == sure[None, :], 1 << 14, lots)
    merit = lots * count + jnp.arange(count)
    return lax.top_k(merit.astype(jnp.int32), top)[1].astype(jnp.int32)


def assign_block(stream_key, own, number, rows, count, top, limit, skew):
    sequence = jax.random.permutation(stream_key, count)
    packed, common = portions_of(count, rows * top, limit, skew, True), portions_of(count, rows * top, limit, skew, False)
    places = jnp.arange(count)

    def named(tallies, turn):
        used = int((tallies > 0).sum())
        fixed = max(1, used // 4)
        passed = fixed + (places - fixed + turn * (used - fixed)) % max(1, count - fixed)
        return jnp.zeros((count,), jnp.int32).at[sequence[jnp.where(places < fixed, places, passed)]].set(jnp.asarray(tallies, jnp.int32))

    tallies = jnp.where(number % 4 == 0, named(packed, number // 4), named(common, number - number // 4 - 1))
    mixed = jax.random.permutation(jax.random.fold_in(own, 3), count)
    donor, receiver = mixed[0:count // 2 * 2:2], mixed[1:count // 2 * 2:2]
    room = jnp.minimum(tallies[donor] - 1, limit - tallies[receiver]) // 2
    room = jnp.where((donor == sequence[0]) | (receiver == sequence[0]) | (tallies[receiver] == 0), 0, jnp.maximum(room, 0))
    passed = jax.random.randint(jax.random.fold_in(own, 4), (count // 2,), 0, 1 << 20) % (room + 1)
    tallies = tallies.at[donor].add(-passed).at[receiver].add(passed)
    labels = jnp.searchsorted(jnp.cumsum(tallies), jnp.arange(rows * top), side="right").astype(jnp.int32)
    grid = labels.reshape(top, rows).T
    grid = grid[jax.random.permutation(jax.random.fold_in(own, 1), rows)]
    turn = jax.random.randint(jax.random.fold_in(own, 2), (rows, 1), 0, top)
    return jnp.take_along_axis(grid, (jnp.arange(top)[None, :] + turn) % top, axis=1)


def portions_of(amount, total, bound, lean, full):
    weights = [(1 << 20) // math.isqrt(grade ** lean) + 1 for grade in range(1, amount + 1)]
    largest = bound if full else min(bound, max(-(-total // amount), total * weights[0] // sum(weights)))
    least = 1 if total - largest >= amount - 1 else 0
    counts, rest = [largest] + [least] * (amount - 1), total - largest - least * (amount - 1)
    while rest > 0:
        free = [i for i in range(1, amount) if counts[i] < largest] or [i for i in range(1, amount) if counts[i] < bound]
        mass, budget = sum([weights[i] for i in free]), rest
        for i in free:
            addition = min(bound - counts[i], max(1, budget * weights[i] // mass), rest)
            counts[i] = counts[i] + addition
            rest = rest - addition
    return np.array(counts)


def bell_draw(own_key, dims, scale, most, cuts=(), held_as=jnp.bfloat16):
    loudness = shard_levels(own_key, dims, cuts, -0.22, 0.18) if cuts else 1.0
    entries = jax.random.normal(own_key, dims, jnp.float32) * scale * loudness
    return jnp.minimum(jnp.maximum(entries, -most), most).astype(held_as)


def setup_inputs(seed: int = 0) -> dict:
    streams_of = jax.random.split(jax.random.key(seed), 11)
    tokens = draw_tokens(jax.random.fold_in(streams_of[10], 71), 0)
    moe_gain = jnp.clip(1.0 + 0.1 * jax.random.normal(streams_of[1], (D,), jnp.float32), 0.5, 1.5).astype(jnp.bfloat16)
    route_ids_keys = jax.random.split(jax.random.fold_in(streams_of[2], 1), TOKENS // TOK_ROW)
    route_ids_turns = jax.random.permutation(jax.random.fold_in(streams_of[2], 3), TOKENS // TOK_ROW)
    route_ids = jax.vmap(lambda own, number: assign_block(jax.random.fold_in(streams_of[2], 2), own, number, TOK_ROW, EXPERTS, TOP, CAP, 2))(route_ids_keys, route_ids_turns).reshape((TOKENS, TOP))
    route_weight = jnp.clip(jnp.exp(math.log(1.0) - 2.3025851 * jax.random.uniform(streams_of[3], (TOKENS, TOP), jnp.float32) ** shard_levels(streams_of[3], (TOKENS, TOP), ((0, 16),), -0.2, 0.2)), 0.1, 1.0)
    w_gate = bell_draw(streams_of[4], (EXPERTS, D, FF), D ** -0.5, 0.109375, ((0, 16), (2, 8)))
    w_up = bell_draw(streams_of[5], (EXPERTS, D, FF), D ** -0.5, 0.109375, ((0, 16), (2, 8)))
    w_down = bell_draw(streams_of[6], (EXPERTS, FF, D), FF ** -0.5, 0.109375, ((0, 16), (1, 8)))
    next_gain = jnp.clip(1.0 + 0.1 * jax.random.normal(streams_of[7], (D,), jnp.float32), 0.5, 1.5).astype(jnp.bfloat16)
    next_gate = draw_next_gate(jax.random.fold_in(streams_of[10], 71), 0)
    next_ids = different_ones(streams_of[9], TOKENS, NEXT_EXPERTS, TOP, 256)
    return dict(tokens=tokens, moe_gain=moe_gain, route_ids=route_ids, route_weight=route_weight, w_gate=w_gate, w_up=w_up, w_down=w_down, next_gain=next_gain, next_gate=next_gate, next_ids=next_ids)


def reference(tokens, moe_gain, route_ids, route_weight, w_gate, w_up, w_down, next_gain, next_gate, next_ids):
    floats = tokens.astype(jnp.float32)
    inverse = lax.rsqrt(lax.optimization_barrier(jnp.mean(floats * floats, axis=-1, keepdims=True)) + 1e-05)
    normed = (floats * inverse * moe_gain.astype(jnp.float32)).astype(jnp.bfloat16)
    gated_in = (floats * inverse * next_gain.astype(jnp.float32)).astype(jnp.bfloat16)
    picks = TOK_ROW * TOP
    blocks = route_ids.reshape(N_ROW, picks)
    onehot = (blocks[:, :, None] == jnp.arange(EXPERTS, dtype=jnp.int32)[None, None, :]).astype(jnp.int32)
    slots = (lax.optimization_barrier(jnp.sum(jnp.cumsum(onehot, axis=1) * onehot, axis=2)) - 1).astype(jnp.int32)
    block_index = jnp.broadcast_to(jnp.arange(N_ROW, dtype=jnp.int32)[:, None], (N_ROW, picks))
    token_of = (block_index * TOK_ROW + jnp.arange(picks, dtype=jnp.int32)[None, :] // TOP).astype(jnp.int32)
    table = jnp.full((EXPERTS, N_ROW, CAP), TOKENS, jnp.int32).at[blocks, block_index, slots].set(token_of)
    padded = jnp.concatenate([normed, jnp.zeros((1, D), jnp.bfloat16)], axis=0)

    def one_expert(inputs):
        index, gate_w, up_w, down_w = inputs
        chosen = padded[index.reshape(-1)].astype(jnp.float32)
        gate = jnp.dot(chosen, gate_w.astype(jnp.float32), preferred_element_type=jnp.float32)
        upward = jnp.dot(chosen, up_w.astype(jnp.float32), preferred_element_type=jnp.float32)
        hidden = (jax.nn.silu(gate) * upward).astype(jnp.bfloat16)
        pieces = jnp.einsum('rcf,cfd->crd', hidden.reshape(-1, N_COL, FF // N_COL).astype(jnp.float32), down_w.reshape(N_COL, FF // N_COL, D).astype(jnp.float32))
        pieces = lax.optimization_barrier(pieces.astype(jnp.bfloat16)).astype(jnp.float32)
        return lax.optimization_barrier(jnp.sum(pieces, axis=0)).astype(jnp.bfloat16)
    outputs = lax.map(one_expert, (table, w_gate, w_up, w_down))
    flat_out = outputs.reshape(EXPERTS * N_ROW * CAP, D)
    where = (blocks * (N_ROW * CAP) + block_index * CAP + slots).astype(jnp.int32)
    gathered = flat_out[where.reshape(-1)].astype(jnp.float32).reshape(TOKENS, TOP, D)
    combined = lax.optimization_barrier(jnp.sum(gathered * route_weight[:, :, None], axis=1))
    mixed = (floats + combined).astype(jnp.bfloat16)
    logits = jnp.dot(gated_in, next_gate, preferred_element_type=jnp.float32)
    highest = lax.optimization_barrier(jnp.max(logits, axis=-1))
    total = lax.optimization_barrier(jnp.sum(jnp.exp(logits - highest[:, None]), axis=-1))
    picked = jnp.take_along_axis(logits, next_ids, axis=1)
    next_logprob = picked - highest[:, None] - jnp.log(total)[:, None]
    return (mixed, next_logprob)
```

```python
import functools

import jax
import jax.numpy as jnp
from jax import lax
from jax.experimental import pallas as pl
from jax.experimental.pallas import tpu as pltpu
from jax.sharding import Mesh
from jax.sharding import PartitionSpec as P

TOP = 4
CAP = 24
COL = ("y", "core")
LANES = 128
VMEM_MB = 56


def params():
    return pltpu.CompilerParams(vmem_limit_bytes=VMEM_MB * 1024 * 1024)


def vmem():
    return pl.BlockSpec(memory_space=pltpu.VMEM)


def smem():
    return pl.BlockSpec(memory_space=pltpu.SMEM)


def round_up(value, step):
    return -(-value // step) * step


def named_by(ids, expert, weight=None):
    total = None
    for k in range(TOP):
        same = ids[k : k + 1, :] == expert
        term = jnp.where(same, 1.0 if weight is None else weight[k : k + 1, :], 0.0)
        total = term if total is None else total + term
    return total


def slot_mask(hot, slot):
    count = hot.shape[1]
    earlier = lax.broadcasted_iota(jnp.int32, (count, count), 0)
    later = lax.broadcasted_iota(jnp.int32, (count, count), 1)
    before = jnp.where(earlier < later, 1.0, 0.0).astype(jnp.bfloat16)
    rank = jnp.dot(hot.astype(jnp.bfloat16), before, preferred_element_type=jnp.float32)
    return jnp.where(rank == slot.astype(jnp.float32), hot, 0.0)


def normalized(tokens, gain):
    floats = tokens.astype(jnp.float32)
    inverse = lax.rsqrt(jnp.mean(floats * floats, axis=0, keepdims=True) + 1e-05)
    return (floats * inverse * gain.astype(jnp.float32)).astype(jnp.bfloat16)


def dot_nt(first, second):
    return lax.dot_general(
        first, second, (((1,), (1,)), ((), ())), preferred_element_type=jnp.float32
    )


def pick_rows(ids, normed, local_expert, local_experts, rows):
    row = lax.broadcasted_iota(jnp.int32, (rows, 1), 0)
    hot = named_by(ids, (row // CAP) * local_experts + local_expert)
    return dot_nt(slot_mask(hot, row % CAP).astype(jnp.bfloat16), normed).astype(jnp.bfloat16)


def dispatch_kernel(local_experts, own_ref, tokens_ref, gain_ref, ids_ref, out_ref):
    normed = normalized(tokens_ref[...], gain_ref[...])
    out_ref[...] = pick_rows(ids_ref[...], normed, own_ref[0], local_experts, out_ref.shape[0])


def route_kernel(
    local_experts, chunks, own_ref, ids_ref, weight_ref, tokens_ref, gain_ref, gate_ref, next_ids_ref,
    high_ref, low_ref, stats_ref,
):
    ids = ids_ref[...]
    weight = weight_ref[...]
    core = own_ref[0]
    rows = high_ref.shape[2]
    row = lax.broadcasted_iota(jnp.int32, (rows, 1), 0)
    other = (row // CAP) % 2
    half = local_experts // 2
    for k in range(chunks):
        expert = (row // (2 * CAP)) * local_experts + (core + other - 2 * core * other) * half + k
        mask = slot_mask(named_by(ids, expert), row % CAP)
        scaled = (named_by(ids, expert, weight) * mask).T
        high = scaled.astype(jnp.bfloat16)
        high_ref[k] = high
        low_ref[k] = (scaled - high.astype(jnp.float32)).astype(jnp.bfloat16)
    gated = normalized(tokens_ref[...], gain_ref[...])
    logits = jnp.dot(gate_ref[...], gated, preferred_element_type=jnp.float32)
    peak = jnp.max(logits, axis=0, keepdims=True)
    total = jnp.sum(jnp.exp(logits - peak), axis=0, keepdims=True)
    column = lax.broadcasted_iota(jnp.int32, logits.shape, 0) + own_ref[1] * logits.shape[0]
    stats_ref[0:1] = peak
    stats_ref[1:2] = total
    for k in range(TOP):
        same = column == next_ids_ref[k : k + 1, :]
        stats_ref[2 + k : 3 + k] = jnp.sum(jnp.where(same, logits, 0.0), axis=0, keepdims=True)
    stats_ref[2 + TOP :] = jnp.zeros((stats_ref.shape[0] - 2 - TOP, logits.shape[1]), jnp.float32)


def expert_kernel(blocks, own_ref, x_ref, gate_ref, up_ref, down_ref, keep_ref, send_ref):
    x = x_ref[...]
    gate = dot_nt(x, gate_ref[0])
    up = dot_nt(x, up_ref[0])
    hidden = (gate / (1.0 + jnp.exp(-gate)) * up).astype(jnp.bfloat16)
    out = jnp.dot(hidden, down_ref[0], preferred_element_type=jnp.float32)
    width = out.shape[1] // blocks
    padded = keep_ref.shape[2]
    rest = jnp.zeros((out.shape[0], padded - width), keep_ref.dtype)

    def store(even_ref, odd_ref):
        for b in range(blocks):
            target = (even_ref, odd_ref)[b % 2]
            target[b // 2, :, :width] = out[:, b * width : (b + 1) * width].astype(target.dtype)
            target[b // 2, :, width:] = rest

    @pl.when(own_ref[1] == 0)
    def _():
        store(keep_ref, send_ref)

    @pl.when(own_ref[1] != 0)
    def _():
        store(send_ref, keep_ref)


def combine_kernel(high_ref, low_ref, rest_ref, *refs):
    parts, out_ref = refs[:-1], refs[-1]
    total = rest_ref[...].astype(jnp.float32)
    width = out_ref.shape[0]
    summed = None
    for k, part_ref in enumerate(parts):
        part = part_ref[...]
        for weight_ref in (high_ref, low_ref):
            term = jnp.dot(weight_ref[k], part, preferred_element_type=jnp.float32)
            summed = term if summed is None else summed + term
    out_ref[...] = (total + summed.T[:width]).astype(out_ref.dtype)


def run_expert(x, w_gate, w_up, w_down, expert, core, blocks, padded):
    rows, features = x.shape
    hidden = w_gate.shape[1]
    out = jax.ShapeDtypeStruct((blocks // 2, rows, padded), jnp.bfloat16)
    whole = lambda *shape: pl.BlockSpec(shape, lambda i, own: (0,) * len(shape))
    return pl.pallas_call(
        functools.partial(expert_kernel, blocks),
        grid_spec=pltpu.PrefetchScalarGridSpec(
            num_scalar_prefetch=1,
            grid=(1,),
            in_specs=[
                whole(rows, features),
                pl.BlockSpec((1, hidden, features), lambda i, own: (own[0], 0, 0)),
                pl.BlockSpec((1, hidden, features), lambda i, own: (own[0], 0, 0)),
                pl.BlockSpec((1, hidden, features), lambda i, own: (own[0], 0, 0)),
            ],
            out_specs=[whole(*out.shape), whole(*out.shape)],
        ),
        out_shape=[out, out],
        compiler_params=params(),
        name="expert",
    )(jnp.stack([expert, core]).astype(jnp.int32), x, w_gate, w_up, w_down)


def swap_cores(x):
    return lax.ppermute(x, "core", [(0, 1), (1, 0)])


def merge_stats(first, second):
    peak = jnp.maximum(first[0:1], second[0:1])
    total = first[1:2] * jnp.exp(first[0:1] - peak) + second[1:2] * jnp.exp(second[0:1] - peak)
    return jnp.concatenate([peak, total, first[2:] + second[2:]], axis=0)


def local(
    tokens, moe_gain, route_ids, route_weight, w_gate, w_up, w_down, next_gain, next_gate, next_ids
):
    row_count = lax.axis_size("row")
    y_count = lax.axis_size("y")
    blocks = 2 * y_count
    tok_rows, features = tokens.shape
    tokens, route_ids, route_weight, next_ids = tokens.T, route_ids.T, route_weight.T, next_ids.T
    next_gate = next_gate.T
    w_gate, w_up = jnp.swapaxes(w_gate, 1, 2), jnp.swapaxes(w_up, 1, 2)
    local_experts = w_gate.shape[0]
    chunks = local_experts // 2
    width = features // blocks
    padded = round_up(width, LANES)
    rows = row_count * CAP
    core = lax.axis_index("core")
    position = lax.axis_index(COL)
    moe_gain = moe_gain.reshape(-1, 1)
    next_gain = next_gain.reshape(-1, 1)

    own = [core * chunks + k for k in range(chunks)]
    others = [(1 - core) * chunks + k for k in range(chunks)]

    def dispatched(k):
        return pl.pallas_call(
            functools.partial(dispatch_kernel, local_experts),
            in_specs=[smem(), vmem(), vmem(), vmem()],
            out_specs=vmem(),
            out_shape=jax.ShapeDtypeStruct((rows, features), jnp.bfloat16),
            compiler_params=params(),
            name="dispatch",
        )(own[k].reshape(1).astype(jnp.int32), tokens, moe_gain, route_ids)

    arrived = []
    for k in range(chunks):
        sent = dispatched(k).reshape(row_count, CAP, features)
        arrived.append(lax.all_to_all(sent, "row", split_axis=0, concat_axis=0, tiled=True))

    table = jax.ShapeDtypeStruct((chunks, tok_rows, 2 * rows), jnp.bfloat16)
    high, low, stats = pl.pallas_call(
        functools.partial(route_kernel, local_experts, chunks),
        in_specs=[smem()] + [vmem()] * 6,
        out_specs=[vmem()] * 3,
        out_shape=[table, table, jax.ShapeDtypeStruct((8, tok_rows), jnp.float32)],
        compiler_params=params(),
        name="route",
    )(jnp.stack([core, position]).astype(jnp.int32), route_ids, route_weight, tokens, next_gain, next_gate, next_ids)

    returned = []
    for k in range(chunks):
        mine = arrived[k]
        theirs = swap_cores(mine)
        keep0, send0 = run_expert(mine.reshape(rows, features), w_gate, w_up, w_down, own[k], core, blocks, padded)
        got0 = swap_cores(send0)
        keep1, send1 = run_expert(theirs.reshape(rows, features), w_gate, w_up, w_down, others[k], core, blocks, padded)
        got1 = swap_cores(send1)
        shape = (y_count, row_count, 1, CAP, padded)
        both = jnp.concatenate(
            [(keep0 + got1).reshape(shape), (keep1 + got0).reshape(shape)], axis=2
        )
        summed = lax.psum_scatter(both, "y", scatter_dimension=0, tiled=True)[0]
        back = lax.all_to_all(summed, "row", split_axis=0, concat_axis=0, tiled=True)
        returned.append(back.reshape(2 * rows, padded))

    merged = merge_stats(stats, swap_cores(stats))
    for step in (1, 2):
        moved = lax.ppermute(merged, "y", [(i, i ^ step) for i in range(y_count)])
        merged = merge_stats(merged, moved)
    next_logprob = (merged[2 : 2 + TOP] - merged[0:1] - jnp.log(merged[1:2])).T

    rest = lax.dynamic_slice_in_dim(tokens, position * width, width, 0)
    mixed = pl.pallas_call(
        combine_kernel,
        in_specs=[vmem()] * (3 + chunks),
        out_specs=vmem(),
        out_shape=jax.ShapeDtypeStruct((width, tok_rows), jnp.bfloat16),
        compiler_params=params(),
        name="combine",
    )(high, low, rest, *returned)
    return (mixed.T, next_logprob)


def solution(mesh):
    torus = Mesh(mesh.devices.reshape(4, 2, mesh.shape["row"]), ("y", "core", "row"))
    return jax.shard_map(
        local,
        mesh=torus,
        in_specs=(
            P("row", None),
            P(),
            P("row", None),
            P("row", None),
            P("row", None, COL),
            P("row", None, COL),
            P("row", COL, None),
            P(),
            P(None, COL),
            P("row", None),
        ),
        out_specs=(P("row", COL), P("row", None)),
        check_vma=False,
    )
```

```python
import functools

import jax
import jax.numpy as jnp
from jax import lax
from jax.experimental import pallas as pl
from jax.experimental.pallas import tpu as pltpu
from jax.sharding import Mesh
from jax.sharding import PartitionSpec as P


TOP = 4
CAP = 24
COL = ("y", "core")
LANES = 128


def params(megabytes=24):
    return pltpu.CompilerParams(vmem_limit_bytes=megabytes * 1024 * 1024)


def vmem():
    return pl.BlockSpec(memory_space=pltpu.VMEM)


def hbm():
    return pl.BlockSpec(memory_space=pltpu.MemorySpace.HBM)


def smem():
    return pl.BlockSpec(memory_space=pltpu.SMEM)


def round_up(value, step):
    return -(-value // step) * step


def named_by(ids, expert, weight=None):
    total = None
    for k in range(TOP):
        same = ids[k : k + 1, :] == expert
        term = jnp.where(same, 1.0 if weight is None else weight[k : k + 1, :], 0.0)
        total = term if total is None else total + term
    return total


def slot_mask(hot, slot):
    count = hot.shape[1]
    earlier = lax.broadcasted_iota(jnp.int32, (count, count), 0)
    later = lax.broadcasted_iota(jnp.int32, (count, count), 1)
    before = jnp.where(earlier < later, 1.0, 0.0).astype(jnp.bfloat16)
    rank = jnp.dot(hot.astype(jnp.bfloat16), before, preferred_element_type=jnp.float32)
    return jnp.where(rank == slot.astype(jnp.float32), hot, 0.0)


def inverse_norm(tokens):
    floats = tokens.astype(jnp.float32)
    return lax.rsqrt(jnp.mean(floats * floats, axis=0, keepdims=True) + 1e-05)


def normalized(tokens, gain):
    scaled = tokens.astype(jnp.float32) * inverse_norm(tokens)
    return (scaled * gain.astype(jnp.float32)).astype(jnp.bfloat16)


def dot_nt(first, second):
    return lax.dot_general(
        first, second, (((1,), (1,)), ((), ())), preferred_element_type=jnp.float32
    )


def dispatch_kernel(local_experts, own_ref, tokens_ref, gain_ref, ids_ref, out_ref):
    tokens = tokens_ref[...]
    rows = out_ref.shape[0]
    row = lax.broadcasted_iota(jnp.int32, (rows, 1), 0)
    hot = named_by(ids_ref[...], (row // CAP) * local_experts + own_ref[0])
    chosen = slot_mask(hot, row % CAP)
    inverse = jnp.sum(chosen * inverse_norm(tokens), axis=1, keepdims=True)
    picked = dot_nt(chosen.astype(jnp.bfloat16), tokens)
    out_ref[...] = (picked * inverse * gain_ref[...].astype(jnp.float32)).astype(jnp.bfloat16)


def route_kernel(
    local_experts, chunks, own_ref, ids_ref, weight_ref, tokens_ref, gain_ref, gate_ref, next_ids_ref,
    high_ref, low_ref, stats_ref,
):
    ids = ids_ref[...]
    weight = weight_ref[...]
    core = own_ref[0]
    rows = high_ref.shape[2]
    row = lax.broadcasted_iota(jnp.int32, (rows, 1), 0)
    other = (row // CAP) % 2
    half = local_experts // 2
    for k in range(chunks):
        expert = (row // (2 * CAP)) * local_experts + (core + other - 2 * core * other) * half + k
        mask = slot_mask(named_by(ids, expert), row % CAP)
        scaled = (named_by(ids, expert, weight) * mask).T
        high = scaled.astype(jnp.bfloat16)
        high_ref[k] = high
        low_ref[k] = (scaled - high.astype(jnp.float32)).astype(jnp.bfloat16)
    gated = normalized(tokens_ref[...], gain_ref[...])
    logits = jnp.dot(gate_ref[...], gated, preferred_element_type=jnp.float32)
    peak = jnp.max(logits, axis=0, keepdims=True)
    total = jnp.sum(jnp.exp(logits - peak), axis=0, keepdims=True)
    column = lax.broadcasted_iota(jnp.int32, logits.shape, 0) + own_ref[1] * logits.shape[0]
    stats_ref[0:1] = peak
    stats_ref[1:2] = total
    for k in range(TOP):
        same = column == next_ids_ref[k : k + 1, :]
        stats_ref[2 + k : 3 + k] = jnp.sum(jnp.where(same, logits, 0.0), axis=0, keepdims=True)
    stats_ref[2 + TOP :] = jnp.zeros((stats_ref.shape[0] - 2 - TOP, logits.shape[1]), jnp.float32)


def expert_kernel(
    blocks, parts, own_ref, x_hbm, gate_hbm, up_hbm, down_hbm, keep_hbm, send_hbm,
    x_ref, gate_ref, up_ref, down_ref, even_ref, odd_ref, in_sems, out_sems,
):
    expert = own_ref[2]
    loads = [
        pltpu.make_async_copy(source, target, in_sems.at[i])
        for i, (source, target) in enumerate(
            (
                (x_hbm, x_ref),
                (gate_hbm.at[expert], gate_ref),
                (up_hbm.at[expert], up_ref),
                (down_hbm.at[expert], down_ref),
            )
        )
    ]
    for load in loads:
        load.start()
    loads[0].wait()
    loads[1].wait()
    x = x_ref[...]
    gate = dot_nt(x, gate_ref[...])
    loads[2].wait()
    up = dot_nt(x, up_ref[...])
    hidden = (gate / (1.0 + jnp.exp(-gate)) * up).astype(jnp.bfloat16)
    loads[3].wait()
    rows, features = x.shape
    around = blocks // 2
    width = features // blocks
    rest = jnp.zeros((rows // parts, even_ref.shape[2] - width), even_ref.dtype)

    def stores(part, even_hbm, odd_hbm):
        here = pl.ds(part * (rows // parts), rows // parts)
        return [
            pltpu.make_async_copy(buf.at[:, here], target.at[:, here], out_sems.at[part, i])
            for i, (buf, target) in enumerate(((even_ref, even_hbm), (odd_ref, odd_hbm)))
        ]

    def each(part, act):
        @pl.when(own_ref[0] == 0)
        def _():
            for copy in stores(part, keep_hbm, send_hbm):
                act(copy)

        @pl.when(own_ref[0] != 0)
        def _():
            for copy in stores(part, send_hbm, keep_hbm):
                act(copy)

    for part in range(parts):
        here = slice(part * (rows // parts), (part + 1) * (rows // parts))
        out = jnp.dot(hidden[here], down_ref[...], preferred_element_type=jnp.float32)
        for b in range(blocks):
            target = (even_ref, odd_ref)[b % 2]
            j = lax.rem(b // 2 - own_ref[1] + around, around)
            target[j, here, :width] = out[:, b * width : (b + 1) * width].astype(target.dtype)
            target[j, here, width:] = rest
        each(part, lambda copy: copy.start())
    for part in range(parts):
        each(part, lambda copy: copy.wait())


def combine_kernel(high_ref, low_ref, part_ref, rest_ref, out_ref):
    part = part_ref[...]
    summed = jnp.dot(high_ref[...], part, preferred_element_type=jnp.float32)
    summed = summed + jnp.dot(low_ref[...], part, preferred_element_type=jnp.float32)
    width = out_ref.shape[0]
    out_ref[...] = (rest_ref[...].astype(jnp.float32) + summed.T[:width]).astype(out_ref.dtype)


def run_expert(x, stacks, place, blocks, padded):
    rows, features = x.shape
    hidden = stacks[0].shape[1]
    parts = 2
    half = (blocks // 2, rows, padded)
    out = jax.ShapeDtypeStruct(half, jnp.bfloat16)
    weight = pltpu.VMEM((hidden, features), jnp.bfloat16)
    return pl.pallas_call(
        functools.partial(expert_kernel, blocks, parts),
        in_specs=[smem()] + [hbm()] * 4,
        out_specs=[hbm(), hbm()],
        out_shape=[out, out],
        scratch_shapes=[
            pltpu.VMEM(x.shape, jnp.bfloat16), weight, weight, weight,
            pltpu.VMEM(half, jnp.bfloat16), pltpu.VMEM(half, jnp.bfloat16),
            pltpu.SemaphoreType.DMA((4,)), pltpu.SemaphoreType.DMA((parts, 2)),
        ],
        compiler_params=params(32),
        name="expert",
    )(place, x, *stacks)


def run_combine(high, low, part, rest, dtype):
    return pl.pallas_call(
        combine_kernel,
        in_specs=[vmem()] * 4,
        out_specs=vmem(),
        out_shape=jax.ShapeDtypeStruct(rest.shape, dtype),
        compiler_params=params(),
        name="combine",
    )(high, low, part, rest)


def swap_cores(x):
    return lax.ppermute(x, "core", [(0, 1), (1, 0)])


def shift_y(x, step):
    count = lax.axis_size("y")
    return lax.ppermute(x, "y", [(i, (i + step) % count) for i in range(count)])


def wide(x):
    return x.astype(jnp.float32)


def reduced_over_y(keep, got):
    half = keep.shape[1] // 2
    pair = lambda j: wide(keep[j]) + wide(got[j])
    far = pair(2).astype(keep.dtype)
    from_low = shift_y(far[:half], 1)
    from_high = shift_y(far[half:], -1)
    up = pair(1)
    down = pair(3)
    up = jnp.concatenate([up[:half] + wide(from_low), up[half:]]).astype(keep.dtype)
    down = jnp.concatenate([down[:half], down[half:] + wide(from_high)]).astype(keep.dtype)
    from_low = shift_y(up, 1)
    from_high = shift_y(down, -1)
    return (pair(0) + wide(from_low) + wide(from_high)).astype(keep.dtype)


def merge_stats(first, second):
    peak = jnp.maximum(first[0:1], second[0:1])
    total = first[1:2] * jnp.exp(first[0:1] - peak) + second[1:2] * jnp.exp(second[0:1] - peak)
    return jnp.concatenate([peak, total, first[2:] + second[2:]], axis=0)


def local(
    tokens, moe_gain, route_ids, route_weight, w_gate, w_up, w_down, next_gain, next_gate, next_ids
):
    row_count = lax.axis_size("row")
    y_count = lax.axis_size("y")
    blocks = 2 * y_count
    tok_rows, features = tokens.shape
    tokens, route_ids, route_weight, next_ids = tokens.T, route_ids.T, route_weight.T, next_ids.T
    next_gate = next_gate.T
    w_gate, w_up = jnp.swapaxes(w_gate, 1, 2), jnp.swapaxes(w_up, 1, 2)
    local_experts = w_gate.shape[0]
    chunks = local_experts // 2
    width = features // blocks
    padded = round_up(width, LANES)
    rows = row_count * CAP
    core = lax.axis_index("core")
    position = lax.axis_index(COL)
    moe_gain = moe_gain.reshape(1, -1)
    next_gain = next_gain.reshape(-1, 1)

    own = [core * chunks + k for k in range(chunks)]
    others = [(1 - core) * chunks + k for k in range(chunks)]
    stacks = tuple(
        pltpu.with_memory_space_constraint(stack, pltpu.MemorySpace.HBM) for stack in (w_gate, w_up, w_down)
    )

    def dispatched(k):
        return pl.pallas_call(
            functools.partial(dispatch_kernel, local_experts),
            in_specs=[smem(), vmem(), vmem(), vmem()],
            out_specs=vmem(),
            out_shape=jax.ShapeDtypeStruct((rows, features), jnp.bfloat16),
            compiler_params=params(),
            name="dispatch",
        )(own[k].reshape(1).astype(jnp.int32), tokens, moe_gain, route_ids)

    arrived = []
    for k in range(chunks):
        sent = dispatched(k).reshape(row_count, CAP, features)
        arrived.append(lax.all_to_all(sent, "row", split_axis=0, concat_axis=0, tiled=True))

    table = jax.ShapeDtypeStruct((chunks, tok_rows, 2 * rows), jnp.bfloat16)
    high, low, stats = pl.pallas_call(
        functools.partial(route_kernel, local_experts, chunks),
        in_specs=[smem()] + [vmem()] * 6,
        out_specs=[vmem()] * 3,
        out_shape=[table, table, jax.ShapeDtypeStruct((8, tok_rows), jnp.float32)],
        compiler_params=params(),
        name="route",
    )(
        jnp.stack([core, position]).astype(jnp.int32),
        route_ids, route_weight, tokens, next_gain, next_gate, next_ids,
    )

    def place(expert):
        return jnp.stack([core, lax.axis_index("y"), expert]).astype(jnp.int32)

    mixed = lax.dynamic_slice_in_dim(tokens, position * width, width, 0)
    for k in range(chunks):
        mine = arrived[k]
        theirs = swap_cores(mine)
        keep0, send0 = run_expert(mine.reshape(rows, features), stacks, place(own[k]), blocks, padded)
        got0 = swap_cores(send0)
        keep1, send1 = run_expert(theirs.reshape(rows, features), stacks, place(others[k]), blocks, padded)
        got1 = swap_cores(send1)
        shape = (y_count, row_count, 1, CAP, padded)
        keep = jnp.concatenate([keep0.reshape(shape), keep1.reshape(shape)], axis=2)
        got = jnp.concatenate([got1.reshape(shape), got0.reshape(shape)], axis=2)
        summed = reduced_over_y(keep, got)
        back = lax.all_to_all(summed, "row", split_axis=0, concat_axis=0, tiled=True)
        dtype = jnp.bfloat16 if k == chunks - 1 else jnp.float32
        mixed = run_combine(high[k], low[k], back.reshape(2 * rows, padded), mixed, dtype)

    merged = merge_stats(stats, swap_cores(stats))
    for step in (1, 2):
        moved = lax.ppermute(merged, "y", [(i, i ^ step) for i in range(y_count)])
        merged = merge_stats(merged, moved)
    next_logprob = (merged[2 : 2 + TOP] - merged[0:1] - jnp.log(merged[1:2])).T
    return (mixed.T, next_logprob)


def solution(mesh):
    torus = Mesh(mesh.devices.reshape(4, 2, mesh.shape["row"]), ("y", "core", "row"))

    return jax.shard_map(
        local,
        mesh=torus,
        in_specs=(
            P("row", None),
            P(),
            P("row", None),
            P("row", None),
            P("row", None, COL),
            P("row", None, COL),
            P("row", COL, None),
            P(),
            P(None, COL),
            P("row", None),
        ),
        out_specs=(P("row", COL), P("row", None)),
        check_vma=False,
    )
```

```python
import functools

import jax
import jax.numpy as jnp
from jax import lax
from jax.experimental import pallas as pl
from jax.experimental.pallas import tpu as pltpu
from jax.sharding import Mesh
from jax.sharding import PartitionSpec as P


TOP = 4
CAP = 24
COL = ("y", "core")
LANES = 128


def params(megabytes=24):
    return pltpu.CompilerParams(vmem_limit_bytes=megabytes * 1024 * 1024)


def vmem():
    return pl.BlockSpec(memory_space=pltpu.VMEM)


def hbm():
    return pl.BlockSpec(memory_space=pltpu.MemorySpace.HBM)


def smem():
    return pl.BlockSpec(memory_space=pltpu.SMEM)


def round_up(value, step):
    return -(-value // step) * step


def named_by(ids, expert, weight=None):
    total = None
    for k in range(TOP):
        same = ids[k : k + 1, :] == expert
        term = jnp.where(same, 1.0 if weight is None else weight[k : k + 1, :], 0.0)
        total = term if total is None else total + term
    return total


def slot_mask(hot, slot):
    count = hot.shape[1]
    earlier = lax.broadcasted_iota(jnp.int32, (count, count), 0)
    later = lax.broadcasted_iota(jnp.int32, (count, count), 1)
    before = jnp.where(earlier < later, 1.0, 0.0).astype(jnp.bfloat16)
    rank = jnp.dot(hot.astype(jnp.bfloat16), before, preferred_element_type=jnp.float32)
    return jnp.where(rank == slot.astype(jnp.float32), hot, 0.0)


def inverse_norm(tokens):
    floats = tokens.astype(jnp.float32)
    return lax.rsqrt(jnp.mean(floats * floats, axis=0, keepdims=True) + 1e-05)


def normalized(tokens, gain):
    scaled = tokens.astype(jnp.float32) * inverse_norm(tokens)
    return (scaled * gain.astype(jnp.float32)).astype(jnp.bfloat16)


def dot_nt(first, second):
    return lax.dot_general(
        first, second, (((1,), (1,)), ((), ())), preferred_element_type=jnp.float32
    )


def dispatch_kernel(local_experts, own_ref, tokens_ref, gain_ref, ids_ref, out_ref):
    tokens = tokens_ref[...]
    rows = out_ref.shape[0]
    row = lax.broadcasted_iota(jnp.int32, (rows, 1), 0)
    hot = named_by(ids_ref[...], (row // CAP) * local_experts + own_ref[0])
    chosen = slot_mask(hot, row % CAP)
    inverse = jnp.sum(chosen * inverse_norm(tokens), axis=1, keepdims=True)
    picked = dot_nt(chosen.astype(jnp.bfloat16), tokens)
    out_ref[...] = (picked * inverse * gain_ref[...].astype(jnp.float32)).astype(jnp.bfloat16)


def route_kernel(
    local_experts, chunks, own_ref, ids_ref, weight_ref, tokens_ref, gain_ref, gate_ref, next_ids_ref,
    high_ref, low_ref, stats_ref,
):
    ids = ids_ref[...]
    weight = weight_ref[...]
    core = own_ref[0]
    rows = high_ref.shape[2]
    row = lax.broadcasted_iota(jnp.int32, (rows, 1), 0)
    other = (row // CAP) % 2
    half = local_experts // 2
    for k in range(chunks):
        expert = (row // (2 * CAP)) * local_experts + (core + other - 2 * core * other) * half + k
        mask = slot_mask(named_by(ids, expert), row % CAP)
        scaled = (named_by(ids, expert, weight) * mask).T
        high = scaled.astype(jnp.bfloat16)
        high_ref[k] = high
        low_ref[k] = (scaled - high.astype(jnp.float32)).astype(jnp.bfloat16)
    gated = normalized(tokens_ref[...], gain_ref[...])
    logits = jnp.dot(gate_ref[...], gated, preferred_element_type=jnp.float32)
    peak = jnp.max(logits, axis=0, keepdims=True)
    total = jnp.sum(jnp.exp(logits - peak), axis=0, keepdims=True)
    column = lax.broadcasted_iota(jnp.int32, logits.shape, 0) + own_ref[1] * logits.shape[0]
    stats_ref[0:1] = peak
    stats_ref[1:2] = total
    for k in range(TOP):
        same = column == next_ids_ref[k : k + 1, :]
        stats_ref[2 + k : 3 + k] = jnp.sum(jnp.where(same, logits, 0.0), axis=0, keepdims=True)
    stats_ref[2 + TOP :] = jnp.zeros((stats_ref.shape[0] - 2 - TOP, logits.shape[1]), jnp.float32)


def expert_kernel(
    blocks, parts, ready, own_ref, x_hbm, gate_in, up_in, down_in, keep_hbm, send_hbm, *refs
):
    expert, following = own_ref[2], own_ref[3]
    weights_in = (gate_in, up_in, down_in)
    if ready:
        x_ref, even_ref, odd_ref, in_sems, out_sems = refs
        weights = weights_in
        loads = []
        fetches = []
    else:
        ahead, refs = refs[:3], refs[3:]
        x_ref, even_ref, odd_ref, in_sems, out_sems = refs[:5]
        weights = refs[5:8]
        loads = [
            pltpu.make_async_copy(source.at[expert], target, in_sems.at[1 + i])
            for i, (source, target) in enumerate(zip(weights_in, weights))
        ]
        fetches = [
            pltpu.make_async_copy(source.at[following], target, in_sems.at[4 + i])
            for i, (source, target) in enumerate(zip(weights_in, ahead))
        ]
    first = pltpu.make_async_copy(x_hbm, x_ref, in_sems.at[0])
    for copy in [first, *loads, *fetches]:
        copy.start()
    rows, features = x_ref.shape
    around = blocks // 2
    width = features // blocks
    size = rows // parts
    rest = jnp.zeros((size, even_ref.shape[2] - width), even_ref.dtype)

    def each(part, act):
        here = pl.ds(part * size, size)

        def both(even_hbm, odd_hbm):
            for i, (buf, target) in enumerate(((even_ref, even_hbm), (odd_ref, odd_hbm))):
                act(pltpu.make_async_copy(buf.at[:, here], target.at[:, here], out_sems.at[part, i]))

        @pl.when(own_ref[0] == 0)
        def _():
            both(keep_hbm, send_hbm)

        @pl.when(own_ref[0] != 0)
        def _():
            both(send_hbm, keep_hbm)

    def weight(i):
        if loads:
            loads[i].wait()
        return weights[i][...]

    first.wait()
    x = x_ref[...]
    gate = dot_nt(x, weight(0))
    up = dot_nt(x, weight(1))
    hidden = (gate / (1.0 + jnp.exp(-gate)) * up).astype(jnp.bfloat16)
    down = weight(2)
    for part in range(parts):
        here = slice(part * size, (part + 1) * size)
        out = jnp.dot(hidden[here], down, preferred_element_type=jnp.float32)
        for b in range(blocks):
            target = (even_ref, odd_ref)[b % 2]
            j = lax.rem(b // 2 - own_ref[1] + around, around)
            target[j, here, :width] = out[:, b * width : (b + 1) * width].astype(target.dtype)
            target[j, here, width:] = rest
        each(part, lambda copy: copy.start())
    for part in range(parts):
        each(part, lambda copy: copy.wait())
    for copy in fetches:
        copy.wait()


def combine_kernel(high_ref, low_ref, part_ref, rest_ref, out_ref):
    part = part_ref[...]
    summed = jnp.dot(high_ref[...], part, preferred_element_type=jnp.float32)
    summed = summed + jnp.dot(low_ref[...], part, preferred_element_type=jnp.float32)
    width = out_ref.shape[0]
    out_ref[...] = (rest_ref[...].astype(jnp.float32) + summed.T[:width]).astype(out_ref.dtype)


def run_expert(x, weights, place, blocks, padded):
    rows, _ = x.shape
    ready = weights[0].ndim == 2
    parts = 2
    half = (blocks // 2, rows, padded)
    out = jax.ShapeDtypeStruct(half, jnp.bfloat16)
    shapes = [] if ready else [pltpu.VMEM(weight.shape[1:], weight.dtype) for weight in weights]
    results = pl.pallas_call(
        functools.partial(expert_kernel, blocks, parts, ready),
        in_specs=[smem(), hbm()] + [vmem() if ready else hbm()] * 3,
        out_specs=[hbm(), hbm()] + [vmem()] * len(shapes),
        out_shape=[out, out] + shapes,
        scratch_shapes=[
            pltpu.VMEM(x.shape, jnp.bfloat16), pltpu.VMEM(half, jnp.bfloat16), pltpu.VMEM(half, jnp.bfloat16),
            pltpu.SemaphoreType.DMA((7,)), pltpu.SemaphoreType.DMA((parts, 2)),
        ] + shapes,
        compiler_params=params(32),
        name="second" if ready else "first",
    )(place, x, *weights)
    return results[0], results[1], results[2:]


def run_combine(high, low, part, rest, dtype):
    return pl.pallas_call(
        combine_kernel,
        in_specs=[vmem()] * 4,
        out_specs=vmem(),
        out_shape=jax.ShapeDtypeStruct(rest.shape, dtype),
        compiler_params=params(),
        name="combine",
    )(high, low, part, rest)


def swap_cores(x):
    return lax.ppermute(x, "core", [(0, 1), (1, 0)])


def shift_y(x, step):
    count = lax.axis_size("y")
    return lax.ppermute(x, "y", [(i, (i + step) % count) for i in range(count)])


def wide(x):
    return x.astype(jnp.float32)


def reduced_over_y(keep, got, shape):
    def pair(keep, got, j):
        parts = [wide(keep[e][j]) + wide(got[1 - e][j]) for e in range(2)]
        return jnp.concatenate([part.reshape(shape) for part in parts], axis=1)

    half = shape[0] // 2
    far = pair(keep, got, 2).astype(jnp.bfloat16)
    keep, got, far = lax.optimization_barrier((keep, got, far))
    from_low = shift_y(far[:half], 1)
    from_high = shift_y(far[half:], -1)
    up = pair(keep, got, 1)
    down = pair(keep, got, 3)
    up = jnp.concatenate([up[:half] + wide(from_low), up[half:]]).astype(jnp.bfloat16)
    down = jnp.concatenate([down[:half], down[half:] + wide(from_high)]).astype(jnp.bfloat16)
    from_low = shift_y(up, 1)
    from_high = shift_y(down, -1)
    return (pair(keep, got, 0) + wide(from_low) + wide(from_high)).astype(jnp.bfloat16)


def merge_stats(first, second):
    peak = jnp.maximum(first[0:1], second[0:1])
    total = first[1:2] * jnp.exp(first[0:1] - peak) + second[1:2] * jnp.exp(second[0:1] - peak)
    return jnp.concatenate([peak, total, first[2:] + second[2:]], axis=0)


def local(
    tokens, moe_gain, route_ids, route_weight, w_gate, w_up, w_down, next_gain, next_gate, next_ids
):
    row_count = lax.axis_size("row")
    y_count = lax.axis_size("y")
    blocks = 2 * y_count
    tok_rows, features = tokens.shape
    tokens, route_ids, route_weight, next_ids = tokens.T, route_ids.T, route_weight.T, next_ids.T
    next_gate = next_gate.T
    w_gate, w_up = jnp.swapaxes(w_gate, 1, 2), jnp.swapaxes(w_up, 1, 2)
    local_experts = w_gate.shape[0]
    chunks = local_experts // 2
    width = features // blocks
    padded = round_up(width, LANES)
    rows = row_count * CAP
    core = lax.axis_index("core")
    position = lax.axis_index(COL)
    moe_gain = moe_gain.reshape(1, -1)
    next_gain = next_gain.reshape(-1, 1)

    own = [core * chunks + k for k in range(chunks)]
    others = [(1 - core) * chunks + k for k in range(chunks)]
    stacks = tuple(
        pltpu.with_memory_space_constraint(stack, pltpu.MemorySpace.HBM) for stack in (w_gate, w_up, w_down)
    )

    def dispatched(k):
        return pl.pallas_call(
            functools.partial(dispatch_kernel, local_experts),
            in_specs=[smem(), vmem(), vmem(), vmem()],
            out_specs=vmem(),
            out_shape=jax.ShapeDtypeStruct((rows, features), jnp.bfloat16),
            compiler_params=params(),
            name="dispatch",
        )(own[k].reshape(1).astype(jnp.int32), tokens, moe_gain, route_ids)

    arrived = []
    for k in range(chunks):
        sent = dispatched(k).reshape(row_count, CAP, features)
        arrived.append(lax.all_to_all(sent, "row", split_axis=0, concat_axis=0, tiled=True))

    table = jax.ShapeDtypeStruct((chunks, tok_rows, 2 * rows), jnp.bfloat16)
    high, low, stats = pl.pallas_call(
        functools.partial(route_kernel, local_experts, chunks),
        in_specs=[smem()] + [vmem()] * 6,
        out_specs=[vmem()] * 3,
        out_shape=[table, table, jax.ShapeDtypeStruct((8, tok_rows), jnp.float32)],
        compiler_params=params(),
        name="route",
    )(
        jnp.stack([core, position]).astype(jnp.int32),
        route_ids, route_weight, tokens, next_gain, next_gate, next_ids,
    )

    def place(k):
        return jnp.stack([core, lax.axis_index("y"), own[k], others[k]]).astype(jnp.int32)

    mixed = lax.dynamic_slice_in_dim(tokens, position * width, width, 0)
    for k in range(chunks):
        mine = arrived[k]
        theirs = swap_cores(mine)
        keep0, send0, ahead = run_expert(mine.reshape(rows, features), stacks, place(k), blocks, padded)
        got0 = swap_cores(send0)
        keep1, send1, _ = run_expert(theirs.reshape(rows, features), ahead, place(k), blocks, padded)
        got1 = swap_cores(send1)
        keep, got = (keep0, keep1), (got0, got1)
        summed = reduced_over_y(keep, got, (row_count, 1, CAP, padded))
        back = lax.all_to_all(summed, "row", split_axis=0, concat_axis=0, tiled=True)
        dtype = jnp.bfloat16 if k == chunks - 1 else jnp.float32
        mixed = run_combine(high[k], low[k], back.reshape(2 * rows, padded), mixed, dtype)

    merged = merge_stats(stats, swap_cores(stats))
    for step in (1, 2):
        moved = lax.ppermute(merged, "y", [(i, i ^ step) for i in range(y_count)])
        merged = merge_stats(merged, moved)
    next_logprob = (merged[2 : 2 + TOP] - merged[0:1] - jnp.log(merged[1:2])).T
    return (mixed.T, next_logprob)


def solution(mesh):
    torus = Mesh(mesh.devices.reshape(4, 2, mesh.shape["row"]), ("y", "core", "row"))

    return jax.shard_map(
        local,
        mesh=torus,
        in_specs=(
            P("row", None),
            P(),
            P("row", None),
            P("row", None),
            P("row", None, COL),
            P("row", None, COL),
            P("row", COL, None),
            P(),
            P(None, COL),
            P("row", None),
        ),
        out_specs=(P("row", COL), P("row", None)),
        check_vma=False,
    )
```

```python
import functools

import jax
import jax.numpy as jnp
from jax import lax
from jax.experimental import pallas as pl
from jax.experimental.pallas import tpu as pltpu
from jax.sharding import Mesh
from jax.sharding import PartitionSpec as P


TOP = 4
CAP = 24
COL = ("y", "core")
DISPATCH_PARTS = 2
LANES = 128


def params(megabytes=24):
    return pltpu.CompilerParams(vmem_limit_bytes=megabytes * 1024 * 1024)


def vmem():
    return pl.BlockSpec(memory_space=pltpu.VMEM)


def hbm():
    return pl.BlockSpec(memory_space=pltpu.MemorySpace.HBM)


def in_hbm(x):
    return pltpu.with_memory_space_constraint(x, pltpu.MemorySpace.HBM)


def smem():
    return pl.BlockSpec(memory_space=pltpu.SMEM)


def round_up(value, step):
    return -(-value // step) * step


def named_by(ids, expert, weight=None):
    total = None
    for k in range(TOP):
        same = ids[k : k + 1, :] == expert
        term = jnp.where(same, 1.0 if weight is None else weight[k : k + 1, :], 0.0)
        total = term if total is None else total + term
    return total


def slot_mask(hot, slot):
    count = hot.shape[1]
    earlier = lax.broadcasted_iota(jnp.int32, (count, count), 0)
    later = lax.broadcasted_iota(jnp.int32, (count, count), 1)
    before = jnp.where(earlier < later, 1.0, 0.0).astype(jnp.bfloat16)
    rank = jnp.dot(hot.astype(jnp.bfloat16), before, preferred_element_type=jnp.float32)
    return jnp.where(rank == slot.astype(jnp.float32), hot, 0.0)


def inverse_norm(tokens):
    floats = tokens.astype(jnp.float32)
    return lax.rsqrt(jnp.mean(floats * floats, axis=0, keepdims=True) + 1e-05)


def normalized(tokens, gain):
    scaled = tokens.astype(jnp.float32) * inverse_norm(tokens)
    return (scaled * gain.astype(jnp.float32)).astype(jnp.bfloat16)


def dot_nt(first, second):
    return lax.dot_general(
        first, second, (((1,), (1,)), ((), ())), preferred_element_type=jnp.float32
    )


def dispatch_kernel(
    local_experts, parts, own_ref, tokens_hbm, gain_ref, ids_hbm, out_hbm,
    tokens_ref, ids_ref, out_ref, in_sems, out_sems,
):
    loads = [
        pltpu.make_async_copy(source, target, in_sems.at[i])
        for i, (source, target) in enumerate(
            ((ids_hbm, ids_ref), (tokens_hbm, tokens_ref))
        )
    ]
    for copy in loads:
        copy.start()
    rows = out_ref.shape[0]
    row = lax.broadcasted_iota(jnp.int32, (rows, 1), 0)
    loads[0].wait()
    hot = named_by(ids_ref[...], (row // CAP) * local_experts + own_ref[0])
    chosen = slot_mask(hot, row % CAP)
    gain = gain_ref[...].astype(jnp.float32)
    loads[1].wait()
    tokens = tokens_ref[...]
    inverse = jnp.sum(chosen * inverse_norm(tokens), axis=1, keepdims=True)
    chosen = chosen.astype(jnp.bfloat16)
    size = rows // parts
    stores = []
    for part in range(parts):
        here = slice(part * size, (part + 1) * size)
        picked = dot_nt(chosen[here], tokens)
        out_ref[here] = (picked * inverse[here] * gain).astype(jnp.bfloat16)
        there = pl.ds(part * size, size)
        stores.append(pltpu.make_async_copy(out_ref.at[there], out_hbm.at[there], out_sems.at[part]))
        stores[-1].start()
    for copy in stores:
        copy.wait()


def route_kernel(
    local_experts, chunks, own_ref, ids_ref, weight_ref, tokens_ref, gain_ref, gate_ref, next_ids_ref,
    high_ref, low_ref, stats_ref,
):
    ids = ids_ref[...]
    weight = weight_ref[...]
    core = own_ref[0]
    rows = high_ref.shape[2]
    row = lax.broadcasted_iota(jnp.int32, (rows, 1), 0)
    other = (row // CAP) % 2
    half = local_experts // 2
    for k in range(chunks):
        expert = (row // (2 * CAP)) * local_experts + (core + other - 2 * core * other) * half + k
        mask = slot_mask(named_by(ids, expert), row % CAP)
        scaled = (named_by(ids, expert, weight) * mask).T
        high = scaled.astype(jnp.bfloat16)
        high_ref[k] = high
        low_ref[k] = (scaled - high.astype(jnp.float32)).astype(jnp.bfloat16)
    gated = normalized(tokens_ref[...], gain_ref[...])
    logits = jnp.dot(gate_ref[...], gated, preferred_element_type=jnp.float32)
    peak = jnp.max(logits, axis=0, keepdims=True)
    total = jnp.sum(jnp.exp(logits - peak), axis=0, keepdims=True)
    column = lax.broadcasted_iota(jnp.int32, logits.shape, 0) + own_ref[1] * logits.shape[0]
    stats_ref[0:1] = peak
    stats_ref[1:2] = total
    for k in range(TOP):
        same = column == next_ids_ref[k : k + 1, :]
        stats_ref[2 + k : 3 + k] = jnp.sum(jnp.where(same, logits, 0.0), axis=0, keepdims=True)
    stats_ref[2 + TOP :] = jnp.zeros((stats_ref.shape[0] - 2 - TOP, logits.shape[1]), jnp.float32)


def expert_kernel(
    blocks, parts, ready, own_ref, x_ref, gate_in, up_in, down_in, keep_hbm, send_hbm, *refs
):
    expert, following = own_ref[2], own_ref[3]
    weights_in = (gate_in, up_in, down_in)
    if ready:
        even_ref, odd_ref, out_sems = refs
        weights = weights_in
        loads = []
        fetches = []
    else:
        ahead, refs = refs[:3], refs[3:]
        even_ref, odd_ref, out_sems, in_sems = refs[:4]
        weights = refs[4:7]
        loads = [
            pltpu.make_async_copy(source.at[expert], target, in_sems.at[i])
            for i, (source, target) in enumerate(zip(weights_in, weights))
        ]
        fetches = [
            pltpu.make_async_copy(source.at[following], target, in_sems.at[3 + i])
            for i, (source, target) in enumerate(zip(weights_in, ahead))
        ]
    for copy in [*loads, *fetches]:
        copy.start()
    rows, features = x_ref.shape
    around = blocks // 2
    width = features // blocks
    size = rows // parts
    rest = jnp.zeros((size, even_ref.shape[2] - width), even_ref.dtype)

    def each(part, act):
        here = pl.ds(part * size, size)

        def both(even_hbm, odd_hbm):
            for i, (buf, target) in enumerate(((even_ref, even_hbm), (odd_ref, odd_hbm))):
                act(pltpu.make_async_copy(buf.at[:, here], target.at[:, here], out_sems.at[part, i]))

        @pl.when(own_ref[0] == 0)
        def _():
            both(keep_hbm, send_hbm)

        @pl.when(own_ref[0] != 0)
        def _():
            both(send_hbm, keep_hbm)

    def weight(i):
        if loads:
            loads[i].wait()
        return weights[i][...]

    x = x_ref[...]
    gate = dot_nt(x, weight(0))
    up = dot_nt(x, weight(1))
    hidden = (gate / (1.0 + jnp.exp(-gate)) * up).astype(jnp.bfloat16)
    down = weight(2)
    for part in range(parts):
        here = slice(part * size, (part + 1) * size)
        out = jnp.dot(hidden[here], down, preferred_element_type=jnp.float32)
        for b in range(blocks):
            target = (even_ref, odd_ref)[b % 2]
            j = lax.rem(b // 2 - own_ref[1] + around, around)
            target[j, here, :width] = out[:, b * width : (b + 1) * width].astype(target.dtype)
            target[j, here, width:] = rest
        each(part, lambda copy: copy.start())
    for part in range(parts):
        each(part, lambda copy: copy.wait())
    for copy in fetches:
        copy.wait()


def combine_kernel(high_ref, low_ref, part_ref, rest_ref, out_ref):
    part = part_ref[...]
    summed = jnp.dot(high_ref[...], part, preferred_element_type=jnp.float32)
    summed = summed + jnp.dot(low_ref[...], part, preferred_element_type=jnp.float32)
    width = out_ref.shape[0]
    out_ref[...] = (rest_ref[...].astype(jnp.float32) + summed.T[:width]).astype(out_ref.dtype)


def run_expert(x, weights, place, blocks, padded):
    rows, _ = x.shape
    ready = weights[0].ndim == 2
    parts = 2
    half = (blocks // 2, rows, padded)
    out = jax.ShapeDtypeStruct(half, jnp.bfloat16)
    shapes = [] if ready else [pltpu.VMEM(weight.shape[1:], weight.dtype) for weight in weights]
    results = pl.pallas_call(
        functools.partial(expert_kernel, blocks, parts, ready),
        in_specs=[smem(), vmem()] + [vmem() if ready else hbm()] * 3,
        out_specs=[hbm(), hbm()] + [vmem()] * len(shapes),
        out_shape=[out, out] + shapes,
        scratch_shapes=[
            pltpu.VMEM(half, jnp.bfloat16), pltpu.VMEM(half, jnp.bfloat16),
            pltpu.SemaphoreType.DMA((parts, 2)),
        ] + ([] if ready else [pltpu.SemaphoreType.DMA((6,))]) + shapes,
        compiler_params=params(32),
        name="second" if ready else "first",
    )(place, x, *weights)
    return results[0], results[1], results[2:]


def run_combine(high, low, part, rest, dtype):
    return pl.pallas_call(
        combine_kernel,
        in_specs=[vmem()] * 4,
        out_specs=vmem(),
        out_shape=jax.ShapeDtypeStruct(rest.shape, dtype),
        compiler_params=params(),
        name="combine",
    )(high, low, part, rest)


def swap_cores(x):
    return lax.ppermute(x, "core", [(0, 1), (1, 0)])


def shift_y(x, step):
    count = lax.axis_size("y")
    return lax.ppermute(x, "y", [(i, (i + step) % count) for i in range(count)])


def wide(x):
    return x.astype(jnp.float32)


def reduced_over_y(keep, got, shape):
    def pair(keep, got, j):
        parts = [wide(keep[e][j]) + wide(got[1 - e][j]) for e in range(2)]
        return jnp.concatenate([part.reshape(shape) for part in parts], axis=1)

    half = shape[0] // 2
    far = pair(keep, got, 2).astype(jnp.bfloat16)
    keep, got, far = lax.optimization_barrier((keep, got, far))
    from_low = shift_y(far[:half], 1)
    from_high = shift_y(far[half:], -1)
    up = pair(keep, got, 1)
    down = pair(keep, got, 3)
    up = jnp.concatenate([up[:half] + wide(from_low), up[half:]]).astype(jnp.bfloat16)
    down = jnp.concatenate([down[:half], down[half:] + wide(from_high)]).astype(jnp.bfloat16)
    from_low = shift_y(up, 1)
    from_high = shift_y(down, -1)
    return (pair(keep, got, 0) + wide(from_low) + wide(from_high)).astype(jnp.bfloat16)


def merge_stats(first, second):
    peak = jnp.maximum(first[0:1], second[0:1])
    total = first[1:2] * jnp.exp(first[0:1] - peak) + second[1:2] * jnp.exp(second[0:1] - peak)
    return jnp.concatenate([peak, total, first[2:] + second[2:]], axis=0)


def local(
    tokens, moe_gain, route_ids, route_weight, w_gate, w_up, w_down, next_gain, next_gate, next_ids
):
    row_count = lax.axis_size("row")
    y_count = lax.axis_size("y")
    blocks = 2 * y_count
    tok_rows, features = tokens.shape
    tokens, route_ids, route_weight, next_ids = tokens.T, route_ids.T, route_weight.T, next_ids.T
    next_gate = next_gate.T
    w_gate, w_up = jnp.swapaxes(w_gate, 1, 2), jnp.swapaxes(w_up, 1, 2)
    local_experts = w_gate.shape[0]
    chunks = local_experts // 2
    width = features // blocks
    padded = round_up(width, LANES)
    rows = row_count * CAP
    core = lax.axis_index("core")
    position = lax.axis_index(COL)
    moe_gain = moe_gain.reshape(1, -1)
    next_gain = next_gain.reshape(-1, 1)

    own = [core * chunks + k for k in range(chunks)]
    others = [(1 - core) * chunks + k for k in range(chunks)]
    stacks = tuple(in_hbm(stack) for stack in (w_gate, w_up, w_down))

    def dispatched(k):
        return pl.pallas_call(
            functools.partial(dispatch_kernel, local_experts, DISPATCH_PARTS),
            in_specs=[smem(), hbm(), vmem(), hbm()],
            out_specs=hbm(),
            out_shape=pltpu.MemorySpace.HBM((rows, features), jnp.bfloat16),
            scratch_shapes=[
                pltpu.VMEM(tokens.shape, tokens.dtype),
                pltpu.VMEM(route_ids.shape, route_ids.dtype), pltpu.VMEM((rows, features), jnp.bfloat16),
                pltpu.SemaphoreType.DMA((2,)), pltpu.SemaphoreType.DMA((DISPATCH_PARTS,)),
            ],
            compiler_params=params(),
            name="dispatch",
        )(own[k].reshape(1).astype(jnp.int32), in_hbm(tokens), moe_gain, in_hbm(route_ids))

    arrived = []
    for k in range(chunks):
        sent = dispatched(k).reshape(row_count, CAP, features)
        arrived.append(lax.all_to_all(sent, "row", split_axis=0, concat_axis=0, tiled=True))

    table = jax.ShapeDtypeStruct((chunks, tok_rows, 2 * rows), jnp.bfloat16)
    high, low, stats = pl.pallas_call(
        functools.partial(route_kernel, local_experts, chunks),
        in_specs=[smem()] + [vmem()] * 6,
        out_specs=[vmem()] * 3,
        out_shape=[table, table, jax.ShapeDtypeStruct((8, tok_rows), jnp.float32)],
        compiler_params=params(),
        name="route",
    )(
        jnp.stack([core, position]).astype(jnp.int32),
        route_ids, route_weight, tokens, next_gain, next_gate, next_ids,
    )

    def place(k):
        return jnp.stack([core, lax.axis_index("y"), own[k], others[k]]).astype(jnp.int32)

    mixed = lax.dynamic_slice_in_dim(tokens, position * width, width, 0)
    for k in range(chunks):
        mine = arrived[k]
        theirs = swap_cores(mine)
        keep0, send0, ahead = run_expert(mine.reshape(rows, features), stacks, place(k), blocks, padded)
        got0 = swap_cores(send0)
        keep1, send1, _ = run_expert(theirs.reshape(rows, features), ahead, place(k), blocks, padded)
        got1 = swap_cores(send1)
        keep, got = (keep0, keep1), (got0, got1)
        summed = reduced_over_y(keep, got, (row_count, 1, CAP, padded))
        back = lax.all_to_all(summed, "row", split_axis=0, concat_axis=0, tiled=True)
        dtype = jnp.bfloat16 if k == chunks - 1 else jnp.float32
        mixed = run_combine(high[k], low[k], back.reshape(2 * rows, padded), mixed, dtype)

    merged = merge_stats(stats, swap_cores(stats))
    for step in (1, 2):
        moved = lax.ppermute(merged, "y", [(i, i ^ step) for i in range(y_count)])
        merged = merge_stats(merged, moved)
    next_logprob = (merged[2 : 2 + TOP] - merged[0:1] - jnp.log(merged[1:2])).T
    return (mixed.T, next_logprob)


def solution(mesh):
    torus = Mesh(mesh.devices.reshape(4, 2, mesh.shape["row"]), ("y", "core", "row"))

    return jax.shard_map(
        local,
        mesh=torus,
        in_specs=(
            P("row", None),
            P(),
            P("row", None),
            P("row", None),
            P("row", None, COL),
            P("row", None, COL),
            P("row", COL, None),
            P(),
            P(None, COL),
            P("row", None),
        ),
        out_specs=(P("row", COL), P("row", None)),
        check_vma=False,
    )
```

```python
import functools

import jax
import jax.numpy as jnp
from jax import lax
from jax.experimental import pallas as pl
from jax.experimental.pallas import tpu as pltpu
from jax.sharding import Mesh
from jax.sharding import PartitionSpec as P


TOP = 4
CAP = 24
COL = ("y", "core")
DISPATCH_PARTS = 2
LANES = 128


def params(megabytes=24):
    return pltpu.CompilerParams(vmem_limit_bytes=megabytes * 1024 * 1024)


def vmem():
    return pl.BlockSpec(memory_space=pltpu.VMEM)


def hbm():
    return pl.BlockSpec(memory_space=pltpu.MemorySpace.HBM)


def in_hbm(x):
    return pltpu.with_memory_space_constraint(x, pltpu.MemorySpace.HBM)


def smem():
    return pl.BlockSpec(memory_space=pltpu.SMEM)


def round_up(value, step):
    return -(-value // step) * step


def named_by(ids, expert, weight=None):
    total = None
    for k in range(TOP):
        same = ids[k : k + 1, :] == expert
        term = jnp.where(same, 1.0 if weight is None else weight[k : k + 1, :], 0.0)
        total = term if total is None else total + term
    return total


def slot_mask(hot, slot):
    count = hot.shape[1]
    earlier = lax.broadcasted_iota(jnp.int32, (count, count), 0)
    later = lax.broadcasted_iota(jnp.int32, (count, count), 1)
    before = jnp.where(earlier < later, 1.0, 0.0).astype(jnp.bfloat16)
    rank = jnp.dot(hot.astype(jnp.bfloat16), before, preferred_element_type=jnp.float32)
    return jnp.where(rank == slot.astype(jnp.float32), hot, 0.0)


def inverse_norm(tokens):
    floats = tokens.astype(jnp.float32)
    return lax.rsqrt(jnp.mean(floats * floats, axis=0, keepdims=True) + 1e-05)


def normalized(tokens, gain):
    scaled = tokens.astype(jnp.float32) * inverse_norm(tokens)
    return (scaled * gain.astype(jnp.float32)).astype(jnp.bfloat16)


def dot_nt(first, second):
    return lax.dot_general(
        first, second, (((1,), (1,)), ((), ())), preferred_element_type=jnp.float32
    )


def dispatch_kernel(
    local_experts, parts, split, own_ref, tokens_hbm, gain_ref, ids_hbm, out_hbm,
    tokens_ref, ids_ref, out_ref, in_sems, out_sems,
):
    loads = [
        pltpu.make_async_copy(source, target, in_sems.at[i])
        for i, (source, target) in enumerate(
            ((ids_hbm, ids_ref), (tokens_hbm, tokens_ref))
        )
    ]
    for copy in loads:
        copy.start()
    rows = out_ref.shape[0]
    row = lax.broadcasted_iota(jnp.int32, (rows, 1), 0)
    loads[0].wait()
    hot = named_by(ids_ref[...], (row // CAP) * local_experts + own_ref[0])
    chosen = slot_mask(hot, row % CAP)
    gain = gain_ref[...].astype(jnp.float32)
    loads[1].wait()
    tokens = tokens_ref[...]
    inverse = jnp.sum(chosen * inverse_norm(tokens), axis=1, keepdims=True)
    chosen = chosen.astype(jnp.bfloat16)
    if split:
        held = out_ref.shape[1]

        def emit(start, count):
            picked = dot_nt(chosen, tokens_ref[start : start + count])
            scaled = picked * inverse * gain[:, start : start + count]
            out_ref[:, :count] = scaled.astype(jnp.bfloat16)
            if count < held:
                out_ref[:, count:] = jnp.zeros((rows, held - count), jnp.bfloat16)

        @pl.when(own_ref[1] == 0)
        def _():
            emit(0, held)

        @pl.when(own_ref[1] != 0)
        def _():
            emit(held, tokens_ref.shape[0] - held)

        parts = 1
    size = rows // parts
    stores = []
    for part in range(parts):
        here = slice(part * size, (part + 1) * size)
        if not split:
            picked = dot_nt(chosen[here], tokens)
            out_ref[here] = (picked * inverse[here] * gain).astype(jnp.bfloat16)
        there = pl.ds(part * size, size)
        stores.append(pltpu.make_async_copy(out_ref.at[there], out_hbm.at[there], out_sems.at[part]))
        stores[-1].start()
    for copy in stores:
        copy.wait()


def route_kernel(
    local_experts, chunks, own_ref, ids_ref, weight_ref, tokens_ref, gain_ref, gate_ref, next_ids_ref,
    high_ref, low_ref, stats_ref,
):
    ids = ids_ref[...]
    weight = weight_ref[...]
    core = own_ref[0]
    rows = high_ref.shape[2]
    row = lax.broadcasted_iota(jnp.int32, (rows, 1), 0)
    other = (row // CAP) % 2
    half = local_experts // 2
    for k in range(chunks):
        expert = (row // (2 * CAP)) * local_experts + (core + other - 2 * core * other) * half + k
        mask = slot_mask(named_by(ids, expert), row % CAP)
        scaled = (named_by(ids, expert, weight) * mask).T
        high = scaled.astype(jnp.bfloat16)
        high_ref[k] = high
        low_ref[k] = (scaled - high.astype(jnp.float32)).astype(jnp.bfloat16)
    gated = normalized(tokens_ref[...], gain_ref[...])
    logits = jnp.dot(gate_ref[...], gated, preferred_element_type=jnp.float32)
    peak = jnp.max(logits, axis=0, keepdims=True)
    total = jnp.sum(jnp.exp(logits - peak), axis=0, keepdims=True)
    column = lax.broadcasted_iota(jnp.int32, logits.shape, 0) + own_ref[1] * logits.shape[0]
    stats_ref[0:1] = peak
    stats_ref[1:2] = total
    for k in range(TOP):
        same = column == next_ids_ref[k : k + 1, :]
        stats_ref[2 + k : 3 + k] = jnp.sum(jnp.where(same, logits, 0.0), axis=0, keepdims=True)
    stats_ref[2 + TOP :] = jnp.zeros((stats_ref.shape[0] - 2 - TOP, logits.shape[1]), jnp.float32)


def expert_kernel(
    blocks, parts, ready, pieces, own_ref, *refs
):
    expert, following = own_ref[2], own_ref[3]
    given, refs = refs[:pieces], refs[pieces:]
    x_ref = given[0]
    if pieces > 1:
        x_ref, refs = refs[-1], refs[:-1]
    weights_in, keep_hbm, send_hbm, refs = refs[:3], refs[3], refs[4], refs[5:]
    loads, fetches = [], []
    if ready:
        even_ref, odd_ref, out_sems = refs
        weights = weights_in
    else:
        ahead, refs = refs[:3], refs[3:]
        even_ref, odd_ref, out_sems, in_sems = refs[:4]
        weights = refs[4:7]
        loads = [
            pltpu.make_async_copy(source.at[expert], target, in_sems.at[i])
            for i, (source, target) in enumerate(zip(weights_in, weights))
        ]
        fetches = [
            pltpu.make_async_copy(source.at[following], target, in_sems.at[3 + i])
            for i, (source, target) in enumerate(zip(weights_in, ahead))
        ]
    for copy in [*loads, *fetches]:
        copy.start()
    if pieces > 1:
        mine, low, high = given
        held = mine.shape[1]
        left = x_ref.shape[1] - held
        middle = low.shape[0]
        odd = lax.rem(own_ref[1], 2)

        @pl.when(odd == 0)
        def _():
            x_ref[:, :held] = mine[...]
            x_ref[:middle, held:] = low[:, :left]
            x_ref[middle:, held:] = high[:, :left]

        @pl.when(odd != 0)
        def _():
            x_ref[:, held:] = mine[:, :left]
            x_ref[:middle, :held] = low[...]
            x_ref[middle:, :held] = high[...]

    rows, features = x_ref.shape
    around = blocks // 2
    width = features // blocks
    size = rows // parts
    rest = jnp.zeros((size, even_ref.shape[2] - width), even_ref.dtype)

    def each(part, act):
        here = pl.ds(part * size, size)

        def both(even_hbm, odd_hbm):
            for i, (buf, target) in enumerate(((even_ref, even_hbm), (odd_ref, odd_hbm))):
                act(pltpu.make_async_copy(buf.at[:, here], target.at[:, here], out_sems.at[part, i]))

        @pl.when(own_ref[0] == 0)
        def _():
            both(keep_hbm, send_hbm)

        @pl.when(own_ref[0] != 0)
        def _():
            both(send_hbm, keep_hbm)

    def weight(i):
        if loads:
            loads[i].wait()
        return weights[i][...]

    x = x_ref[...]
    gate = dot_nt(x, weight(0))
    up = dot_nt(x, weight(1))
    hidden = (gate / (1.0 + jnp.exp(-gate)) * up).astype(jnp.bfloat16)
    down = weight(2)
    for part in range(parts):
        here = slice(part * size, (part + 1) * size)
        out = jnp.dot(hidden[here], down, preferred_element_type=jnp.float32)
        for b in range(blocks):
            target = (even_ref, odd_ref)[b % 2]
            j = lax.rem(b // 2 - own_ref[1] + around, around)
            target[j, here, :width] = out[:, b * width : (b + 1) * width].astype(target.dtype)
            target[j, here, width:] = rest
        each(part, lambda copy: copy.start())
    for part in range(parts):
        each(part, lambda copy: copy.wait())
    for copy in fetches:
        copy.wait()


def combine_kernel(high_ref, low_ref, part_ref, rest_ref, out_ref):
    part = part_ref[...]
    summed = jnp.dot(high_ref[...], part, preferred_element_type=jnp.float32)
    summed = summed + jnp.dot(low_ref[...], part, preferred_element_type=jnp.float32)
    width = out_ref.shape[0]
    out_ref[...] = (rest_ref[...].astype(jnp.float32) + summed.T[:width]).astype(out_ref.dtype)


def run_expert(x, weights, place, blocks, padded):
    rows = x[0].shape[0]
    features = weights[0].shape[-1]
    ready = weights[0].ndim == 2
    parts = 2
    half = (blocks // 2, rows, padded)
    out = jax.ShapeDtypeStruct(half, jnp.bfloat16)
    shapes = [] if ready else [pltpu.VMEM(weight.shape[1:], weight.dtype) for weight in weights]
    results = pl.pallas_call(
        functools.partial(expert_kernel, blocks, parts, ready, len(x)),
        in_specs=[smem()] + [vmem()] * len(x) + [vmem() if ready else hbm()] * 3,
        out_specs=[hbm(), hbm()] + [vmem()] * len(shapes),
        out_shape=[out, out] + shapes,
        scratch_shapes=[
            pltpu.VMEM(half, jnp.bfloat16), pltpu.VMEM(half, jnp.bfloat16),
            pltpu.SemaphoreType.DMA((parts, 2)),
        ] + ([] if ready else [pltpu.SemaphoreType.DMA((6,))]) + shapes
        + ([pltpu.VMEM((rows, features), jnp.bfloat16)] if len(x) > 1 else []),
        compiler_params=params(32),
        name="second" if ready else "first",
    )(place, *x, *weights)
    return results[0], results[1], results[2:]


def run_combine(high, low, part, rest, dtype):
    return pl.pallas_call(
        combine_kernel,
        in_specs=[vmem()] * 4,
        out_specs=vmem(),
        out_shape=jax.ShapeDtypeStruct(rest.shape, dtype),
        compiler_params=params(),
        name="combine",
    )(high, low, part, rest)


def swap_cores(x):
    return lax.ppermute(x, "core", [(0, 1), (1, 0)])


def shift_y(x, step):
    count = lax.axis_size("y")
    return lax.ppermute(x, "y", [(i, (i + step) % count) for i in range(count)])


def wide(x):
    return x.astype(jnp.float32)


def reduced_over_y(keep, got, shape):
    def pair(keep, got, j):
        parts = [wide(keep[e][j]) + wide(got[1 - e][j]) for e in range(2)]
        return jnp.concatenate([part.reshape(shape) for part in parts], axis=1)

    half = shape[0] // 2
    far = pair(keep, got, 2).astype(jnp.bfloat16)
    keep, got, far = lax.optimization_barrier((keep, got, far))
    from_low = shift_y(far[:half], 1)
    from_high = shift_y(far[half:], -1)
    up = pair(keep, got, 1)
    down = pair(keep, got, 3)
    up = jnp.concatenate([up[:half] + wide(from_low), up[half:]]).astype(jnp.bfloat16)
    down = jnp.concatenate([down[:half], down[half:] + wide(from_high)]).astype(jnp.bfloat16)
    from_low = shift_y(up, 1)
    from_high = shift_y(down, -1)
    return (pair(keep, got, 0) + wide(from_low) + wide(from_high)).astype(jnp.bfloat16)


def merge_stats(first, second):
    peak = jnp.maximum(first[0:1], second[0:1])
    total = first[1:2] * jnp.exp(first[0:1] - peak) + second[1:2] * jnp.exp(second[0:1] - peak)
    return jnp.concatenate([peak, total, first[2:] + second[2:]], axis=0)


def local(
    tokens, moe_gain, route_ids, route_weight, w_gate, w_up, w_down, next_gain, next_gate, next_ids
):
    row_count = lax.axis_size("row")
    y_count = lax.axis_size("y")
    blocks = 2 * y_count
    tok_rows, features = tokens.shape
    tokens, route_ids, route_weight, next_ids = tokens.T, route_ids.T, route_weight.T, next_ids.T
    next_gate = next_gate.T
    w_gate, w_up = jnp.swapaxes(w_gate, 1, 2), jnp.swapaxes(w_up, 1, 2)
    local_experts = w_gate.shape[0]
    chunks = local_experts // 2
    width = features // blocks
    padded = round_up(width, LANES)
    rows = row_count * CAP
    core = lax.axis_index("core")
    position = lax.axis_index(COL)
    moe_gain = moe_gain.reshape(1, -1)
    next_gain = next_gain.reshape(-1, 1)

    own = [core * chunks + k for k in range(chunks)]
    others = [(1 - core) * chunks + k for k in range(chunks)]
    stacks = tuple(in_hbm(stack) for stack in (w_gate, w_up, w_down))

    held = round_up(features // 2, 2 * LANES)
    odd = lax.axis_index("y") % 2

    def dispatched(k):
        share = held if k == 0 else features
        return pl.pallas_call(
            functools.partial(dispatch_kernel, local_experts, DISPATCH_PARTS, k == 0),
            in_specs=[smem(), hbm(), vmem(), hbm()],
            out_specs=hbm(),
            out_shape=pltpu.MemorySpace.HBM((rows, share), jnp.bfloat16),
            scratch_shapes=[
                pltpu.VMEM(tokens.shape, tokens.dtype),
                pltpu.VMEM(route_ids.shape, route_ids.dtype), pltpu.VMEM((rows, share), jnp.bfloat16),
                pltpu.SemaphoreType.DMA((2,)), pltpu.SemaphoreType.DMA((DISPATCH_PARTS,)),
            ],
            compiler_params=params(),
            name="dispatch",
        )(jnp.stack([own[k], odd]).astype(jnp.int32), in_hbm(tokens), moe_gain, in_hbm(route_ids))

    arrived = []
    for k in range(chunks):
        sent = dispatched(k).reshape(row_count, CAP, -1)
        arrived.append(lax.all_to_all(sent, "row", split_axis=0, concat_axis=0, tiled=True))

    table = jax.ShapeDtypeStruct((chunks, tok_rows, 2 * rows), jnp.bfloat16)
    high, low, stats = pl.pallas_call(
        functools.partial(route_kernel, local_experts, chunks),
        in_specs=[smem()] + [vmem()] * 6,
        out_specs=[vmem()] * 3,
        out_shape=[table, table, jax.ShapeDtypeStruct((8, tok_rows), jnp.float32)],
        compiler_params=params(),
        name="route",
    )(
        jnp.stack([core, position]).astype(jnp.int32),
        route_ids, route_weight, tokens, next_gain, next_gate, next_ids,
    )

    def place(k):
        return jnp.stack([core, lax.axis_index("y"), own[k], others[k]]).astype(jnp.int32)

    mixed = lax.dynamic_slice_in_dim(tokens, position * width, width, 0)
    for k in range(chunks):
        mine = [arrived[k]]
        if k == 0:
            half = row_count // 2
            mine += [shift_y(mine[0][:half], 1), shift_y(mine[0][half:], -1)]
        theirs = [swap_cores(piece) for piece in mine]
        flat = lambda pieces: [piece.reshape(-1, piece.shape[-1]) for piece in pieces]
        keep0, send0, ahead = run_expert(flat(mine), stacks, place(k), blocks, padded)
        got0 = swap_cores(send0)
        keep1, send1, _ = run_expert(flat(theirs), ahead, place(k), blocks, padded)
        got1 = swap_cores(send1)
        keep, got = (keep0, keep1), (got0, got1)
        summed = reduced_over_y(keep, got, (row_count, 1, CAP, padded))
        back = lax.all_to_all(summed, "row", split_axis=0, concat_axis=0, tiled=True)
        dtype = jnp.bfloat16 if k == chunks - 1 else jnp.float32
        mixed = run_combine(high[k], low[k], back.reshape(2 * rows, padded), mixed, dtype)

    merged = merge_stats(stats, swap_cores(stats))
    for step in (1, 2):
        moved = lax.ppermute(merged, "y", [(i, i ^ step) for i in range(y_count)])
        merged = merge_stats(merged, moved)
    next_logprob = (merged[2 : 2 + TOP] - merged[0:1] - jnp.log(merged[1:2])).T
    return (mixed.T, next_logprob)


def solution(mesh):
    torus = Mesh(mesh.devices.reshape(4, 2, mesh.shape["row"]), ("y", "core", "row"))

    return jax.shard_map(
        local,
        mesh=torus,
        in_specs=(
            P("row", None),
            P(),
            P("row", None),
            P("row", None),
            P("row", None, COL),
            P("row", None, COL),
            P("row", COL, None),
            P(),
            P(None, COL),
            P("row", None),
        ),
        out_specs=(P("row", COL), P("row", None)),
        check_vma=False,
    )
```

```python
import functools

import jax
import jax.numpy as jnp
from jax import lax
from jax.experimental import pallas as pl
from jax.experimental.pallas import tpu as pltpu
from jax.sharding import Mesh
from jax.sharding import PartitionSpec as P


TOP = 4
CAP = 24
COL = ("y", "core")
DISPATCH_PARTS = 2
LANES = 128


def params(megabytes=24):
    return pltpu.CompilerParams(vmem_limit_bytes=megabytes * 1024 * 1024)


def vmem():
    return pl.BlockSpec(memory_space=pltpu.VMEM)


def hbm():
    return pl.BlockSpec(memory_space=pltpu.MemorySpace.HBM)


def in_hbm(x):
    return pltpu.with_memory_space_constraint(x, pltpu.MemorySpace.HBM)


def smem():
    return pl.BlockSpec(memory_space=pltpu.SMEM)


def round_up(value, step):
    return -(-value // step) * step


def named_by(ids, expert, weight=None):
    total = None
    for k in range(TOP):
        same = ids[k : k + 1, :] == expert
        term = jnp.where(same, 1.0 if weight is None else weight[k : k + 1, :], 0.0)
        total = term if total is None else total + term
    return total


def slot_mask(hot, slot):
    count = hot.shape[1]
    earlier = lax.broadcasted_iota(jnp.int32, (count, count), 0)
    later = lax.broadcasted_iota(jnp.int32, (count, count), 1)
    before = jnp.where(earlier < later, 1.0, 0.0).astype(jnp.bfloat16)
    rank = jnp.dot(hot.astype(jnp.bfloat16), before, preferred_element_type=jnp.float32)
    return jnp.where(rank == slot.astype(jnp.float32), hot, 0.0)


def inverse_norm(tokens):
    floats = tokens.astype(jnp.float32)
    return lax.rsqrt(jnp.mean(floats * floats, axis=0, keepdims=True) + 1e-05)


def normalized(tokens, gain):
    scaled = tokens.astype(jnp.float32) * inverse_norm(tokens)
    return (scaled * gain.astype(jnp.float32)).astype(jnp.bfloat16)


def dot_nt(first, second):
    return lax.dot_general(
        first, second, (((1,), (1,)), ((), ())), preferred_element_type=jnp.float32
    )


def dispatch_kernel(
    local_experts, parts, split, own_ref, tokens_hbm, gain_ref, ids_hbm, out_hbm,
    tokens_ref, ids_ref, out_ref, in_sems, out_sems,
):
    loads = [
        pltpu.make_async_copy(source, target, in_sems.at[i])
        for i, (source, target) in enumerate(
            ((ids_hbm, ids_ref), (tokens_hbm, tokens_ref))
        )
    ]
    for copy in loads:
        copy.start()
    rows = out_ref.shape[0]
    row = lax.broadcasted_iota(jnp.int32, (rows, 1), 0)
    loads[0].wait()
    hot = named_by(ids_ref[...], (row // CAP) * local_experts + own_ref[0])
    chosen = slot_mask(hot, row % CAP)
    gain = gain_ref[...].astype(jnp.float32)
    loads[1].wait()
    tokens = tokens_ref[...]
    inverse = jnp.sum(chosen * inverse_norm(tokens), axis=1, keepdims=True)
    chosen = chosen.astype(jnp.bfloat16)
    if split:
        held = out_ref.shape[1]

        def emit(start, count):
            picked = dot_nt(chosen, tokens_ref[start : start + count])
            scaled = picked * inverse * gain[:, start : start + count]
            out_ref[:, :count] = scaled.astype(jnp.bfloat16)
            if count < held:
                out_ref[:, count:] = jnp.zeros((rows, held - count), jnp.bfloat16)

        @pl.when(own_ref[1] == 0)
        def _():
            emit(0, held)

        @pl.when(own_ref[1] != 0)
        def _():
            emit(held, tokens_ref.shape[0] - held)

        parts = 1
    size = rows // parts
    stores = []
    for part in range(parts):
        here = slice(part * size, (part + 1) * size)
        if not split:
            picked = dot_nt(chosen[here], tokens)
            out_ref[here] = (picked * inverse[here] * gain).astype(jnp.bfloat16)
        there = pl.ds(part * size, size)
        stores.append(pltpu.make_async_copy(out_ref.at[there], out_hbm.at[there], out_sems.at[part]))
        stores[-1].start()
    for copy in stores:
        copy.wait()


def route_kernel(
    local_experts, chunks, own_ref, ids_ref, weight_ref, tokens_ref, gain_ref, gate_ref, next_ids_ref,
    high_ref, low_ref, stats_ref,
):
    ids = ids_ref[...]
    weight = weight_ref[...]
    core = own_ref[0]
    rows = high_ref.shape[2]
    row = lax.broadcasted_iota(jnp.int32, (rows, 1), 0)
    other = (row // CAP) % 2
    half = local_experts // 2
    for k in range(chunks):
        expert = (row // (2 * CAP)) * local_experts + (core + other - 2 * core * other) * half + k
        mask = slot_mask(named_by(ids, expert), row % CAP)
        scaled = (named_by(ids, expert, weight) * mask).T
        high = scaled.astype(jnp.bfloat16)
        high_ref[k] = high
        low_ref[k] = (scaled - high.astype(jnp.float32)).astype(jnp.bfloat16)
    gated = normalized(tokens_ref[...], gain_ref[...])
    logits = jnp.dot(gate_ref[...], gated, preferred_element_type=jnp.float32)
    peak = jnp.max(logits, axis=0, keepdims=True)
    total = jnp.sum(jnp.exp(logits - peak), axis=0, keepdims=True)
    column = lax.broadcasted_iota(jnp.int32, logits.shape, 0) + own_ref[1] * logits.shape[0]
    stats_ref[0:1] = peak
    stats_ref[1:2] = total
    for k in range(TOP):
        same = column == next_ids_ref[k : k + 1, :]
        stats_ref[2 + k : 3 + k] = jnp.sum(jnp.where(same, logits, 0.0), axis=0, keepdims=True)
    stats_ref[2 + TOP :] = jnp.zeros((stats_ref.shape[0] - 2 - TOP, logits.shape[1]), jnp.float32)


def expert_kernel(
    blocks, parts, ready, pieces, own_ref, *refs
):
    expert, following = own_ref[2], own_ref[3]
    given, refs = refs[:pieces], refs[pieces:]
    x_ref = given[0]
    if pieces > 1:
        x_ref, refs = refs[-1], refs[:-1]
    weights_in, keep_hbm, send_hbm, refs = refs[:3], refs[3], refs[4], refs[5:]
    loads, fetches = [], []
    if ready:
        even_ref, odd_ref, out_sems = refs
        weights = weights_in
    else:
        ahead, refs = refs[:3], refs[3:]
        even_ref, odd_ref, out_sems, in_sems = refs[:4]
        weights = refs[4:7]
        loads = [
            pltpu.make_async_copy(source.at[expert], target, in_sems.at[i])
            for i, (source, target) in enumerate(zip(weights_in, weights))
        ]
        fetches = [
            pltpu.make_async_copy(source.at[following], target, in_sems.at[3 + i])
            for i, (source, target) in enumerate(zip(weights_in, ahead))
        ]
    for copy in [*loads, *fetches]:
        copy.start()
    if pieces > 1:
        mine, low, high = given
        held = mine.shape[1]
        left = x_ref.shape[1] - held
        middle = low.shape[0]
        odd = lax.rem(own_ref[1], 2)

        @pl.when(odd == 0)
        def _():
            x_ref[:, :held] = mine[...]
            x_ref[:middle, held:] = low[:, :left]
            x_ref[middle:, held:] = high[:, :left]

        @pl.when(odd != 0)
        def _():
            x_ref[:, held:] = mine[:, :left]
            x_ref[:middle, :held] = low[...]
            x_ref[middle:, :held] = high[...]

    rows, features = x_ref.shape
    around = blocks // 2
    width = features // blocks
    size = rows // parts
    rest = jnp.zeros((size, even_ref.shape[2] - width), even_ref.dtype)

    def each(part, act):
        here = pl.ds(part * size, size)

        def both(even_hbm, odd_hbm):
            for i, (buf, target) in enumerate(((even_ref, even_hbm), (odd_ref, odd_hbm))):
                act(pltpu.make_async_copy(buf.at[:, here], target.at[:, here], out_sems.at[part, i]))

        @pl.when(own_ref[0] == 0)
        def _():
            both(keep_hbm, send_hbm)

        @pl.when(own_ref[0] != 0)
        def _():
            both(send_hbm, keep_hbm)

    def weight(i):
        if loads:
            loads[i].wait()
        return weights[i][...]

    x = x_ref[...]
    gate = dot_nt(x, weight(0))
    up = dot_nt(x, weight(1))
    hidden = (gate / (1.0 + jnp.exp(-gate)) * up).astype(jnp.bfloat16)
    down = weight(2)
    for part in range(parts):
        here = slice(part * size, (part + 1) * size)
        out = jnp.dot(hidden[here], down, preferred_element_type=jnp.float32)
        for b in range(blocks):
            target = (even_ref, odd_ref)[b % 2]
            j = lax.rem(b // 2 - own_ref[1] + around, around)
            target[j, here, :width] = out[:, b * width : (b + 1) * width].astype(target.dtype)
            target[j, here, width:] = rest
        each(part, lambda copy: copy.start())
    for part in range(parts):
        each(part, lambda copy: copy.wait())
    for copy in fetches:
        copy.wait()


def combine_kernel(high_ref, low_ref, part_ref, rest_ref, out_ref):
    part = part_ref[...]
    summed = jnp.dot(high_ref[...], part, preferred_element_type=jnp.float32)
    summed = summed + jnp.dot(low_ref[...], part, preferred_element_type=jnp.float32)
    width = out_ref.shape[0]
    out_ref[...] = (rest_ref[...].astype(jnp.float32) + summed.T[:width]).astype(out_ref.dtype)


def run_expert(x, weights, place, blocks, padded):
    rows = x[0].shape[0]
    features = weights[0].shape[-1]
    ready = weights[0].ndim == 2
    parts = 2
    half = (blocks // 2, rows, padded)
    out = jax.ShapeDtypeStruct(half, jnp.bfloat16)
    shapes = [] if ready else [pltpu.VMEM(weight.shape[1:], weight.dtype) for weight in weights]
    results = pl.pallas_call(
        functools.partial(expert_kernel, blocks, parts, ready, len(x)),
        in_specs=[smem()] + [vmem()] * len(x) + [vmem() if ready else hbm()] * 3,
        out_specs=[hbm(), hbm()] + [vmem()] * len(shapes),
        out_shape=[out, out] + shapes,
        scratch_shapes=[
            pltpu.VMEM(half, jnp.bfloat16), pltpu.VMEM(half, jnp.bfloat16),
            pltpu.SemaphoreType.DMA((parts, 2)),
        ] + ([] if ready else [pltpu.SemaphoreType.DMA((6,))]) + shapes
        + ([pltpu.VMEM((rows, features), jnp.bfloat16)] if len(x) > 1 else []),
        compiler_params=params(32),
        name="second" if ready else "first",
    )(place, *x, *weights)
    return results[0], results[1], results[2:]


def run_combine(high, low, part, rest, dtype):
    return pl.pallas_call(
        combine_kernel,
        in_specs=[vmem()] * 4,
        out_specs=vmem(),
        out_shape=jax.ShapeDtypeStruct(rest.shape, dtype),
        compiler_params=params(),
        name="combine",
    )(high, low, part, rest)


def swap_cores(x):
    return lax.ppermute(x, "core", [(0, 1), (1, 0)])


def shift_y(x, step):
    count = lax.axis_size("y")
    return lax.ppermute(x, "y", [(i, (i + step) % count) for i in range(count)])


def wide(x):
    return x.astype(jnp.float32)


def reduced_over_y(keep, got, shape):
    def pair(keep, got, j):
        parts = [wide(keep[e][j]) + wide(got[1 - e][j]) for e in range(2)]
        return jnp.concatenate([part.reshape(shape) for part in parts], axis=1)

    half = shape[0] // 2
    narrow = lambda x: x.astype(jnp.bfloat16)
    far, up, down = (pair(keep, got, j) for j in (2, 1, 3))
    rising = narrow(jnp.stack([far[:half], up[half:]]))
    falling = narrow(jnp.stack([far[half:], down[:half]]))
    keep, got, rising, falling = lax.optimization_barrier((keep, got, rising, falling))
    low = shift_y(rising, 1)
    high = shift_y(falling, -1)
    up = narrow(pair(keep, got, 1)[:half] + wide(low[0]))
    down = narrow(pair(keep, got, 3)[half:] + wide(high[0]))
    last_low = shift_y(up, 1)
    last_high = shift_y(down, -1)
    own = pair(keep, got, 0)
    first = own[:half] + wide(high[1]) + wide(last_low)
    second = own[half:] + wide(low[1]) + wide(last_high)
    return narrow(jnp.concatenate([first, second]))


def merge_stats(first, second):
    peak = jnp.maximum(first[0:1], second[0:1])
    total = first[1:2] * jnp.exp(first[0:1] - peak) + second[1:2] * jnp.exp(second[0:1] - peak)
    return jnp.concatenate([peak, total, first[2:] + second[2:]], axis=0)


def local(
    tokens, moe_gain, route_ids, route_weight, w_gate, w_up, w_down, next_gain, next_gate, next_ids
):
    row_count = lax.axis_size("row")
    y_count = lax.axis_size("y")
    blocks = 2 * y_count
    tok_rows, features = tokens.shape
    tokens, route_ids, route_weight, next_ids = tokens.T, route_ids.T, route_weight.T, next_ids.T
    next_gate = next_gate.T
    w_gate, w_up = jnp.swapaxes(w_gate, 1, 2), jnp.swapaxes(w_up, 1, 2)
    local_experts = w_gate.shape[0]
    chunks = local_experts // 2
    width = features // blocks
    padded = round_up(width, LANES)
    rows = row_count * CAP
    core = lax.axis_index("core")
    position = lax.axis_index(COL)
    moe_gain = moe_gain.reshape(1, -1)
    next_gain = next_gain.reshape(-1, 1)

    own = [core * chunks + k for k in range(chunks)]
    others = [(1 - core) * chunks + k for k in range(chunks)]
    stacks = tuple(in_hbm(stack) for stack in (w_gate, w_up, w_down))

    held = round_up(features // 2, 2 * LANES)
    odd = lax.axis_index("y") % 2

    def dispatched(k):
        share = held if k == 0 else features
        return pl.pallas_call(
            functools.partial(dispatch_kernel, local_experts, DISPATCH_PARTS, k == 0),
            in_specs=[smem(), hbm(), vmem(), hbm()],
            out_specs=hbm(),
            out_shape=pltpu.MemorySpace.HBM((rows, share), jnp.bfloat16),
            scratch_shapes=[
                pltpu.VMEM(tokens.shape, tokens.dtype),
                pltpu.VMEM(route_ids.shape, route_ids.dtype), pltpu.VMEM((rows, share), jnp.bfloat16),
                pltpu.SemaphoreType.DMA((2,)), pltpu.SemaphoreType.DMA((DISPATCH_PARTS,)),
            ],
            compiler_params=params(),
            name="dispatch",
        )(jnp.stack([own[k], odd]).astype(jnp.int32), in_hbm(tokens), moe_gain, in_hbm(route_ids))

    arrived = []
    for k in range(chunks):
        sent = dispatched(k).reshape(row_count, CAP, -1)
        arrived.append(lax.all_to_all(sent, "row", split_axis=0, concat_axis=0, tiled=True))

    table = jax.ShapeDtypeStruct((chunks, tok_rows, 2 * rows), jnp.bfloat16)
    high, low, stats = pl.pallas_call(
        functools.partial(route_kernel, local_experts, chunks),
        in_specs=[smem()] + [vmem()] * 6,
        out_specs=[vmem()] * 3,
        out_shape=[table, table, jax.ShapeDtypeStruct((8, tok_rows), jnp.float32)],
        compiler_params=params(),
        name="route",
    )(
        jnp.stack([core, position]).astype(jnp.int32),
        route_ids, route_weight, tokens, next_gain, next_gate, next_ids,
    )

    def place(k):
        return jnp.stack([core, lax.axis_index("y"), own[k], others[k]]).astype(jnp.int32)

    mixed = lax.dynamic_slice_in_dim(tokens, position * width, width, 0)
    for k in range(chunks):
        mine = [arrived[k]]
        if k == 0:
            half = row_count // 2
            mine += [shift_y(mine[0][:half], 1), shift_y(mine[0][half:], -1)]
        theirs = [swap_cores(piece) for piece in mine]
        flat = lambda pieces: [piece.reshape(-1, piece.shape[-1]) for piece in pieces]
        keep0, send0, ahead = run_expert(flat(mine), stacks, place(k), blocks, padded)
        got0 = swap_cores(send0)
        keep1, send1, _ = run_expert(flat(theirs), ahead, place(k), blocks, padded)
        got1 = swap_cores(send1)
        keep, got = (keep0, keep1), (got0, got1)
        summed = reduced_over_y(keep, got, (row_count, 1, CAP, padded))
        back = lax.all_to_all(summed, "row", split_axis=0, concat_axis=0, tiled=True)
        dtype = jnp.bfloat16 if k == chunks - 1 else jnp.float32
        mixed = run_combine(high[k], low[k], back.reshape(2 * rows, padded), mixed, dtype)

    merged = merge_stats(stats, swap_cores(stats))
    for step in (1, 2):
        moved = lax.ppermute(merged, "y", [(i, i ^ step) for i in range(y_count)])
        merged = merge_stats(merged, moved)
    next_logprob = (merged[2 : 2 + TOP] - merged[0:1] - jnp.log(merged[1:2])).T
    return (mixed.T, next_logprob)


def solution(mesh):
    torus = Mesh(mesh.devices.reshape(4, 2, mesh.shape["row"]), ("y", "core", "row"))

    return jax.shard_map(
        local,
        mesh=torus,
        in_specs=(
            P("row", None),
            P(),
            P("row", None),
            P("row", None),
            P("row", None, COL),
            P("row", None, COL),
            P("row", COL, None),
            P(),
            P(None, COL),
            P("row", None),
        ),
        out_specs=(P("row", COL), P("row", None)),
        check_vma=False,
    )
```
